512 devices in a mesh: batch: 8 (over y_lo, x), rows: 8 (over z), chan: 8 (over y_hi, core).
Axes of the slice: x: 4, y: 8 (y_hi: 4, y_lo: 2; y = y_hi * 2 + y_lo), z: 8, core: 2. Of those that a mesh axis runs over, the one named last changes fastest.
Arguments:
- images: float32 [64, 24, 64, 32], P('batch', None, ('rows', 'chan')), may hold values from -6 to 6
- shift_mid: float32 [3, 24], replicated, may hold values from -1.75 to 1.75
- gain_mid: float32 [3, 24], replicated, may hold values from -0.3 to 0.3
- lower_mid: float32 [3, 24, 24], replicated, may hold values from -1.25 to 1.25
- upper_mid: float32 [3, 24, 24], replicated, may hold values from -1.25 to 1.25
- diag_mid: float32 [3, 24], replicated, may hold values from -0.3 to 0.3
- first_mid: bfloat16 [3, 9, 12, 512], replicated, may hold values from -0.625 to 0.625
- first_bias_mid: bfloat16 [3, 512], replicated, may hold values from -3 to 3
- second_mid: bfloat16 [3, 512, 512], replicated, may hold values from -0.25 to 0.25
- second_bias_mid: float32 [3, 512], replicated, may hold values from -3 to 3
- third_mid: bfloat16 [3, 9, 512, 24], replicated, may hold values from -0.09375 to 0.09375
- third_bias_mid: float32 [3, 24], replicated, may hold values from -3 to 3
- shift_top: float32 [2, 48], replicated, may hold values from -1.75 to 1.75
- gain_top: float32 [2, 48], replicated, may hold values from -0.3 to 0.3
- lower_top: float32 [2, 48, 48], replicated, may hold values from -0.875 to 0.875
- upper_top: float32 [2, 48, 48], replicated, may hold values from -0.875 to 0.875
- diag_top: float32 [2, 48], replicated, may hold values from -0.3 to 0.3
- first_top: bfloat16 [2, 9, 24, 512], replicated, may hold values from -0.4375 to 0.4375
- first_bias_top: bfloat16 [2, 512], replicated, may hold values from -3 to 3
- second_top: bfloat16 [2, 512, 512], replicated, may hold values from -0.25 to 0.25
- second_bias_top: float32 [2, 512], replicated, may hold values from -3 to 3
- third_top: bfloat16 [2, 9, 512, 48], replicated, may hold values from -0.09375 to 0.09375
- third_bias_top: float32 [2, 48], replicated, may hold values from -3 to 3
Outputs:
- latent_mid: float32 [64, 12, 64, 32], P('batch', None, ('rows', 'chan'))
- latent_top: float32 [64, 48, 32, 16], P(('batch', 'chan'), None, 'rows')
- loglik: float32 [64], P(('batch', 'chan'))
The draws below stay inside these ranges and needn't reach their ends.
All inputs are finite; a program needn't handle non-finite values.
Results may differ from the reference program's by a relative error of at most 0.008.
Values may be sent and summed in bfloat16 or wider, within the bound.
No kernel may reach another device: no remote copies, remote signals or barrier semaphores. Data moves between devices by JAX's collectives and lax.ppermute only.
A program may use at most 64 MiB of HBM per device.

```python
import math
import jax
import jax.numpy as jnp
from jax import lax

HID = 512
C2 = 24
W2 = 32
STEPS2 = 3
STEPS3 = 2
B = 64
H2 = 64
C3 = 48


def level_of(rng, extent, split, least, high):
    gain, own = 1.0, jax.random.fold_in(rng, 6)
    for axis_at, shards_of in split:
        draws = jnp.exp(jax.random.uniform(jax.random.fold_in(own, axis_at), (shards_of,), jnp.float32, least / len(split), high / len(split)))
        gain = gain * jnp.repeat(draws, extent[axis_at] // shards_of).reshape([-1 if axis == axis_at else 1 for axis in range(len(extent))])
    return gain


def centred(rng, dims, width, bound, shards=(), held_as=jnp.bfloat16):
    array = width * jax.random.normal(rng, dims, jnp.float32)
    if shards:
        array = array * level_of(rng, dims, shards, -0.22, 0.18)
    return jnp.clip(array, -bound, bound).astype(held_as)


def setup_inputs(seed: int = 0) -> dict:
    keys = jax.random.split(jax.random.key(seed), 24)
    return {
        "images": centred(keys[0], (B, C2, H2, W2), 1.0, 6.0, ((0, 8), (2, 64)), jnp.float32),
        "shift_mid": centred(keys[1], (STEPS2, C2), 0.3, 1.75, (), jnp.float32),
        "gain_mid": jnp.clip(jax.random.uniform(keys[2], (STEPS2, C2), jnp.float32, -0.3, 0.3), -0.3, 0.3),
        "lower_mid": centred(keys[3], (STEPS2, C2, C2), C2 ** -0.5, 1.25, (), jnp.float32),
        "upper_mid": centred(keys[4], (STEPS2, C2, C2), C2 ** -0.5, 1.25, (), jnp.float32),
        "diag_mid": jnp.clip(jax.random.uniform(keys[5], (STEPS2, C2), jnp.float32, -0.3, 0.3), -0.3, 0.3),
        "first_mid": centred(keys[6], (STEPS2, 9, C2 // 2, HID), (9 * C2 // 2) ** -0.5, 0.625),
        "first_bias_mid": centred(keys[7], (STEPS2, HID), 0.5, 3.0),
        "second_mid": centred(keys[8], (STEPS2, HID, HID), HID ** -0.5, 0.25),
        "second_bias_mid": centred(keys[9], (STEPS2, HID), 0.5, 3.0, (), jnp.float32),
        "third_mid": centred(keys[10], (STEPS2, 9, HID, C2), (9 * HID) ** -0.5, 0.09375),
        "third_bias_mid": centred(keys[11], (STEPS2, C2), 0.5, 3.0, (), jnp.float32),
        "shift_top": centred(keys[12], (STEPS3, C3), 0.3, 1.75, (), jnp.float32),
        "gain_top": jnp.clip(jax.random.uniform(keys[13], (STEPS3, C3), jnp.float32, -0.3, 0.3), -0.3, 0.3),
        "lower_top": centred(keys[14], (STEPS3, C3, C3), C3 ** -0.5, 0.875, (), jnp.float32),
        "upper_top": centred(keys[15], (STEPS3, C3, C3), C3 ** -0.5, 0.875, (), jnp.float32),
        "diag_top": jnp.clip(jax.random.uniform(keys[16], (STEPS3, C3), jnp.float32, -0.3, 0.3), -0.3, 0.3),
        "first_top": centred(keys[17], (STEPS3, 9, C2, HID), (9 * C2) ** -0.5, 0.4375),
        "first_bias_top": centred(keys[18], (STEPS3, HID), 0.5, 3.0),
        "second_top": centred(keys[19], (STEPS3, HID, HID), HID ** -0.5, 0.25),
        "second_bias_top": centred(keys[20], (STEPS3, HID), 0.5, 3.0, (), jnp.float32),
        "third_top": centred(keys[21], (STEPS3, 9, HID, C3), (9 * HID) ** -0.5, 0.09375),
        "third_bias_top": centred(keys[22], (STEPS3, C3), 0.5, 3.0, (), jnp.float32),
    }


log_two_pi = math.log(2.0 * math.pi)


def spatial_conv(source, weights):
    height = source.shape[1]
    columns = source.shape[2]
    padded = jnp.pad(source, ((0, 0), (1, 1), (1, 1))).astype(jnp.float32)
    summed = jnp.zeros((weights.shape[2], height, columns), jnp.float32)
    for tap_idx in range(9):
        row_off = tap_idx // 3
        col_off = tap_idx % 3
        window = padded[:, row_off:row_off + height, col_off:col_off + columns]
        summed = summed + jnp.einsum('chw,co->ohw', window, weights[tap_idx].astype(jnp.float32))
    return summed


def flow_step(flow_state, params):
    shift_vec, gain_vec, lower_raw, upper_raw, diag_log, first_w, first_b, second_w, second_b, third_w, third_b = params
    channels = flow_state.shape[0]
    half_chan = channels // 2
    cell_count = flow_state.shape[1] * flow_state.shape[2]
    mixed_state = (flow_state + shift_vec[:, None, None]) * jnp.exp(gain_vec)[:, None, None]
    lower_mat = jnp.tril(lower_raw, -1) + jnp.eye(channels, dtype=jnp.float32)
    upper_mat = jnp.triu(upper_raw, 1) + jnp.diag(jnp.exp(diag_log))
    matrix = jnp.dot(lower_mat, upper_mat, precision=lax.Precision.HIGHEST)
    mixed_state = jnp.einsum('oc,chw->ohw', matrix, mixed_state, precision=lax.Precision.HIGHEST)
    part_a = mixed_state[:half_chan]
    part_b = mixed_state[half_chan:]
    coupled = part_a.astype(jnp.bfloat16)
    inner = jax.nn.relu(spatial_conv(coupled, first_w) + first_b.astype(jnp.float32)[:, None, None]).astype(jnp.bfloat16)
    middle = jnp.einsum('chw,co->ohw', inner.astype(jnp.float32), second_w.astype(jnp.float32))
    middle = jax.nn.relu(middle + second_b[:, None, None]).astype(jnp.bfloat16)
    output = spatial_conv(middle, third_w) + third_b[:, None, None]
    gate_pre = output[:half_chan] + 2.0
    updated = (part_b + output[half_chan:]) * jax.nn.sigmoid(gate_pre)
    step_term = cell_count * (jnp.sum(gain_vec) + jnp.sum(diag_log)) + jnp.sum(jax.nn.log_sigmoid(gate_pre))
    return jnp.concatenate([part_a, updated], axis=0), step_term


def image_flow(picture, params_mid, params_top):
    flow_state = picture
    logdet = jnp.zeros((), jnp.float32)
    for step_num in range(params_mid[0].shape[0]):
        flow_state, step_term = flow_step(flow_state, tuple(p[step_num] for p in params_mid))
        logdet = logdet + step_term
    half_chan = flow_state.shape[0] // 2
    latent_mid = flow_state[:half_chan]
    kept_chan = flow_state[half_chan:]
    count_chan, height, columns = kept_chan.shape
    squeezed = kept_chan.reshape(count_chan, height // 2, 2, columns // 2, 2).transpose(0, 2, 4, 1, 3)
    flow_state = squeezed.reshape(count_chan * 4, height // 2, columns // 2)
    for step_num in range(params_top[0].shape[0]):
        flow_state, step_term = flow_step(flow_state, tuple(p[step_num] for p in params_top))
        logdet = logdet + step_term
    latent_top = flow_state
    latent_count = latent_mid.size + latent_top.size
    logprob = -0.5 * (jnp.sum(latent_mid * latent_mid) + jnp.sum(latent_top * latent_top)) - 0.5 * log_two_pi * latent_count
    total_dims = picture.shape[0] * picture.shape[1] * picture.shape[2]
    return latent_mid, latent_top, (logprob + logdet) / total_dims


def reference(images, shift_mid, gain_mid, lower_mid, upper_mid, diag_mid, first_mid, first_bias_mid, second_mid, second_bias_mid, third_mid, third_bias_mid, shift_top, gain_top, lower_top, upper_top, diag_top, first_top, first_bias_top, second_top, second_bias_top, third_top, third_bias_top):
    params_mid = (shift_mid, gain_mid, lower_mid, upper_mid, diag_mid, first_mid, first_bias_mid, second_mid, second_bias_mid, third_mid, third_bias_mid)
    params_top = (shift_top, gain_top, lower_top, upper_top, diag_top, first_top, first_bias_top, second_top, second_bias_top, third_top, third_bias_top)
    latent_mid, latent_top, loglik = lax.map(lambda picture: image_flow(picture, params_mid, params_top), images)
    return (latent_mid, latent_top, loglik)
```

```python
import functools
import math

import jax
import jax.numpy as jnp
from jax import lax
from jax.experimental import pallas as pl
from jax.experimental.pallas import tpu as pltpu
from jax.sharding import PartitionSpec as P

BF = jnp.bfloat16
F32 = jnp.float32
log_two_pi = math.log(2.0 * math.pi)
VMEM = pl.BlockSpec(memory_space=pltpu.VMEM)
SMEM = pl.BlockSpec(memory_space=pltpu.SMEM)


def iota(shape, dim):
    return lax.broadcasted_iota(jnp.int32, shape, dim)


def eye(n, dtype):
    return (iota((n, n), 0) == iota((n, n), 1)).astype(dtype)


def dot_t(a, b):
    return lax.dot_general(a, b, (((1,), (1,)), ((), ())), preferred_element_type=F32)


def dot(a, b):
    return jnp.dot(a, b, preferred_element_type=F32)


def halves(x):
    high = x.astype(BF)
    return high, (x - high.astype(F32)).astype(BF)


def to_column(row):
    n = row.shape[1]
    same = iota((n, n), 0) == iota((n, n), 1)
    return jnp.sum(jnp.where(same, row, 0.0), axis=1, keepdims=True)


def three_term_left(matrix):
    high, low = halves(matrix)
    return jnp.concatenate([high, high, low], axis=1)


def select_rows(n_out, n_in, source_of):
    return (iota((n_out, n_in), 1) == source_of(iota((n_out, n_in), 0))).astype(F32)


def spread_mid(o):
    return jnp.where(o < 12, o, jnp.where(o >= 20, o - 8, -1))


def flow_matrix(gain, lower, upper, diag, shift, n):
    i, j = iota((n, n), 0), iota((n, n), 1)
    low = jnp.where(i > j, lower, 0.0) + jnp.where(i == j, 1.0, 0.0)
    up = jnp.where(i < j, upper, 0.0) + jnp.where(i == j, jnp.exp(diag), 0.0)
    matrix = jnp.dot(low, up, precision=lax.Precision.HIGHEST, preferred_element_type=F32)
    matrix = matrix * jnp.exp(gain)
    return matrix, jnp.sum(matrix * shift, axis=1, keepdims=True)


def exact_dot(a, b):
    return jnp.dot(a, b, precision=lax.Precision.HIGHEST, preferred_element_type=F32)


def prep_kernel(
    shift_mid, gain_mid, lower_mid, upper_mid, diag_mid, first_mid, first_bias_mid, second_mid,
    second_bias_mid, third_mid, third_bias_mid,
    shift_top, gain_top, lower_top, upper_top, diag_top, first_top, first_bias_top, second_top,
    second_bias_top, third_top, third_bias_top,
    a_mid, bu_mid, w1_mid, w2_mid, b2_mid, w3_mid, b3_mid,
    a_top0, a_top1, bu_top, w1_top, w2_top, b2_top, w3_top, b3_top, const,
):
    hid = second_mid.shape[1]
    ident = eye(hid, BF)
    total = jnp.zeros((1, 1), F32)
    for s in range(3):
        row = slice(s, s + 1)
        matrix, offset = flow_matrix(gain_mid[row], lower_mid[s], upper_mid[s], diag_mid[row], shift_mid[row], 24)
        total = total + 2048.0 * jnp.sum(gain_mid[row] + diag_mid[row], axis=1, keepdims=True)
        rows = select_rows(32, 24, spread_mid)
        matrix = exact_dot(rows, matrix)
        offset = jnp.sum(rows * jnp.sum(jnp.where(eye(24, F32) > 0, offset, 0.0), axis=0, keepdims=True), axis=1, keepdims=True)
        offset = offset + (iota((32, 1), 0) == 12).astype(F32)
        if s == 0:
            columns = (iota((24, 32), 0) == iota((24, 32), 1)).astype(F32)
        else:
            columns = (iota((24, 32), 0) == spread_mid(iota((24, 32), 1))).astype(F32)
        a_mid[s] = three_term_left(exact_dot(matrix, columns))
        bu_mid[s] = jnp.broadcast_to(offset, (32, 128))
        zeros = jnp.zeros((4, hid), F32)
        with_bias = jnp.concatenate([first_bias_mid[row].astype(F32), zeros[:3]], axis=0)
        blocks = []
        for tap in range(9):
            blocks += [first_mid[s, tap].astype(F32), with_bias if tap == 4 else zeros]
        w1_mid[s] = dot_t(ident, jnp.concatenate(blocks, axis=0).astype(BF)).astype(BF)
        w2_mid[s] = dot_t(ident, second_mid[s]).astype(BF)
        b2_mid[s] = jnp.broadcast_to(second_bias_mid[row], (128, hid)).T
        for tap in range(9):
            w3_mid[s, 24 * tap : 24 * tap + 24, :] = dot_t(eye(24, BF), third_mid[s, tap]).astype(BF)
        b3 = to_column(third_bias_mid[row]) + jnp.where(iota((24, 1), 0) < 12, 2.0, 0.0)
        b3_mid[s] = jnp.broadcast_to(b3, (24, 128))
    for s in range(2):
        row = slice(s, s + 1)
        matrix, offset = flow_matrix(gain_top[row], lower_top[s], upper_top[s], diag_top[row], shift_top[row], 48)
        total = total + 512.0 * jnp.sum(gain_top[row] + diag_top[row], axis=1, keepdims=True)
        if s == 0:
            k = iota((48, 64), 1)
            source = jnp.where(k % 16 >= 4, 4 * (k % 16 - 4) + k // 16, -1)
            a_top0[...] = three_term_left(exact_dot(matrix, (iota((48, 64), 0) == source).astype(F32)))
        else:
            a_top1[...] = three_term_left(matrix)
        bu_top[s] = jnp.broadcast_to(offset, (48, 128))
        blocks = [first_top[s, tap].astype(F32) for tap in range(9)]
        blocks += [first_bias_top[row].astype(F32), jnp.zeros((7, hid), F32)]
        w1_top[s] = dot_t(ident, jnp.concatenate(blocks, axis=0).astype(BF)).astype(BF)
        w2_top[s] = dot_t(ident, second_top[s]).astype(BF)
        b2_top[s] = jnp.broadcast_to(second_bias_top[row], (128, hid)).T
        for tap in range(9):
            w3_top[s, 48 * tap : 48 * tap + 48, :] = dot_t(eye(48, BF), third_top[s, tap]).astype(BF)
        b3 = to_column(third_bias_top[row]) + jnp.where(iota((48, 1), 0) < 24, 2.0, 0.0)
        b3_top[s] = jnp.broadcast_to(b3, (48, 128))
    const[...] = jnp.broadcast_to(total, (8, 128))


def tiled(column, lanes):
    return jnp.concatenate([column] * (lanes // 128), axis=1)


def moved(x, by):
    lanes = x.shape[1]
    return pltpu.roll(x, (-by) % lanes, 1)


def row_moved(x, dr, width):
    if dr == 0:
        return x
    lane = iota(x.shape, 1)
    inside = lane >= width if dr < 0 else lane < x.shape[1] - width
    return jnp.where(inside, moved(x, dr * width), 0.0)


def column_moved(x, dc, width):
    if dc == 0:
        return x
    column = iota(x.shape, 1) % width
    inside = column >= 1 if dc < 0 else column <= width - 2
    return jnp.where(inside, moved(x, dc), 0.0)


def conditioner(q, extra, w1, w2, b2, w3, b3, x_scr, p_scr, width, chunk):
    cells = q.shape[1]
    rows = q.shape[0]
    sides = [column_moved(q, dc, width) for dc in (-1, 0, 1)]
    blocks = [row_moved(side, dr, width) for dr in (-1, 0, 1) for side in sides]
    if extra is not None:
        blocks.append(extra)
    x_scr[...] = jnp.concatenate(blocks, axis=0).astype(BF)
    bias = tiled(b2, chunk)

    def one(i):
        at = pl.ds(i * chunk, chunk)
        inner = jnp.maximum(dot(w1, x_scr[:, at]), 0.0).astype(BF)
        middle = jnp.maximum(dot(w2, inner) + bias, 0.0).astype(BF)
        p_scr[:, at] = dot(w3, middle)

    for i in range(cells // chunk):
        one(i)
    n_out = p_scr.shape[0] // 9
    out = tiled(b3, cells)
    for dc in (-1, 0, 1):
        part = None
        for dr in (-1, 0, 1):
            tap = 3 * (dr + 1) + dc + 1
            term = row_moved(p_scr[n_out * tap : n_out * (tap + 1), :], dr, width)
            part = term if part is None else part + term
        out = out + column_moved(part, dc, width)
    return out


def gate_of(g):
    e = jnp.exp(-jnp.abs(g))
    scale = 1.0 / (1.0 + e)
    return jnp.where(g >= 0.0, scale, e * scale), jnp.minimum(g, 0.0) - jnp.log(1.0 + e)


def mix(a, parts, bias):
    return dot(a, jnp.concatenate(parts, axis=0)) + bias


def mid_update(u, s, refs, x_scr, p_scr):
    w1, w2, b2, w3, b3 = refs
    out = conditioner(u[:16], None, w1[s], w2[s], b2[s], w3[s], b3[s], x_scr, p_scr, 32, 512)
    scale, logs = gate_of(out[:16])
    logs = jnp.where(iota(logs.shape, 0) < 12, logs, 0.0)
    updated = (u[16:] + out[8:]) * pltpu.roll(scale, 4, 0)
    return updated, jnp.sum(logs, keepdims=True)


def mid_kernel(slots, where, a_mid, bu_mid, w1, w2, b2, w3, b3, u_out, sum_out, latent_out, x_scr, p_scr):
    refs = (w1, w2, b2, w3, b3)
    cells = 2048
    lane = iota((8, 128), 1) // 32
    groups = []
    for g in range(3):
        pieces = []
        for k in range(16):
            piece = None
            for j in range(4):
                source = slots[4 * k + j]
                turn = (32 * (j - g)) % 128
                source = pltpu.roll(source, turn, 1) if turn else source
                piece = source if piece is None else jnp.where(lane == j, source, piece)
            pieces.append(piece)
        groups.append(jnp.concatenate(pieces, axis=1))
    state = jnp.concatenate(groups + [jnp.zeros((8, cells), F32)], axis=0)
    total = jnp.zeros((1, 1), F32)
    for s in range(2):
        high, low = halves(state)
        u = mix(a_mid[s], [high, low, high], tiled(bu_mid[s], cells))
        updated, logs = mid_update(u, s, refs, x_scr, p_scr)
        total = total + logs
        state = jnp.concatenate([u[:16], updated], axis=0)
    high, low = halves(state)
    u = mix(a_mid[2], [high, low, high], tiled(bu_mid[2], cells))
    u_out[...] = u
    latent = jnp.where(iota((16, cells), 0) < 12, u[:16], 0.0)
    total = total - 0.5 * jnp.sum(latent * latent, keepdims=True)
    sum_out[...] = jnp.broadcast_to(total, (8, 128))
    own = u_out[0:16, pl.ds(pl.multiple_of(where[0] * 256, 256), 256)]
    for j in range(8):
        latent_out[j] = own[:12, 32 * j : 32 * j + 32]


def top_kernel(u_in, sum_in, where, const, w1m, w2m, b2m, w3m, b3m, a_top0, a_top1, bu_top, w1, w2, b2, w3, b3,
               latent_out, sum_out, x_scr, p_scr, xt_scr, pt_scr):
    updated, logs = mid_update(u_in[...], 2, (w1m, w2m, b2m, w3m, b3m), x_scr, p_scr)
    total = sum_in[0:1, 0:1] + const[0:1, 0:1] + logs
    high, low = halves(updated)
    cell = iota((128, 128), 0)
    target = 32 * (2 * (cell // 32 % 2) + cell % 2) + 16 * (cell // 64) + cell % 32 // 2
    order = (target == iota((128, 128), 1)).astype(BF)
    stacked = jnp.concatenate([part[:, 128 * k : 128 * k + 128] for part in (high, low) for k in range(16)], axis=0)
    stacked = dot(stacked, order)
    lane = iota((16, 128), 1) // 32
    parts = []
    for p in range(2):
        for ij in range(4):
            pieces = []
            for m in range(4):
                piece = None
                for j in range(4):
                    start = 256 * p + 16 * (4 * m + j)
                    source = stacked[start : start + 16]
                    turn = (32 * (j - ij)) % 128
                    source = pltpu.roll(source, turn, 1) if turn else source
                    piece = source if piece is None else jnp.where(lane == j, source, piece)
                pieces.append(piece)
            parts.append(jnp.concatenate(pieces, axis=1).astype(BF))
    u = mix(a_top0[...], parts + parts[:4], tiled(bu_top[0], 512))
    ones = (iota((8, 512), 0) == 0).astype(F32)
    for s in range(2):
        out = conditioner(u[:24], ones, w1[s], w2[s], b2[s], w3[s], b3[s], xt_scr, pt_scr, 16, 512)
        scale, logs = gate_of(out[:24])
        total = total + jnp.sum(logs, keepdims=True)
        state = jnp.concatenate([u[:24], (u[24:] + out[24:]) * scale], axis=0)
        if s == 0:
            high, low = halves(state)
            u = mix(a_top1[...], [high, low, high], tiled(bu_top[1], 512))
    total = total - 0.5 * jnp.sum(state * state, keepdims=True)
    total = (total - 0.5 * log_two_pi * 49152.0) * (1.0 / 49152.0)
    sum_out[...] = jnp.broadcast_to(total, (8, 128))
    block = pltpu.roll(state, (512 - where[0] * 64) % 512, 1)
    latent_out[...] = block[:, :64]


def pack_kernel(images, packed):
    for i in range(8):
        rows = images[i]
        wide = jnp.concatenate([rows[0:8], rows[8:16], rows[16:24], jnp.zeros((8, 32), F32)], axis=1)
        for r in range(8):
            packed[8 * r + i] = wide


def shapes(*items):
    return tuple(jax.ShapeDtypeStruct(shape, dtype) for shape, dtype in items)


def body(images, *params):
    picked = pl.pallas_call(
        pack_kernel, in_specs=[VMEM], out_specs=VMEM, out_shape=jax.ShapeDtypeStruct((64, 8, 128), F32), name="pack"
    )(images.reshape(8, 24, 32))
    slots = lax.all_to_all(picked, ("rows", "chan"), 0, 0, tiled=True)
    prepared = pl.pallas_call(
        prep_kernel,
        in_specs=[VMEM] * 22,
        out_specs=(VMEM,) * 16,
        out_shape=shapes(
            ((3, 32, 96), BF), ((3, 32, 128), F32), ((3, 512, 144), BF), ((3, 512, 512), BF), ((3, 512, 128), F32),
            ((3, 216, 512), BF), ((3, 24, 128), F32),
            ((48, 192), BF), ((48, 144), BF), ((2, 48, 128), F32), ((2, 512, 224), BF), ((2, 512, 512), BF),
            ((2, 512, 128), F32), ((2, 432, 512), BF), ((2, 48, 128), F32), ((8, 128), F32),
        ),
        name="prep",
    )(*params)
    a_mid, bu_mid, *mid = prepared[:7]
    *top, const = prepared[7:]
    where = lax.axis_index("rows").astype(jnp.int32).reshape(1)
    u, sums, latent = pl.pallas_call(
        mid_kernel,
        in_specs=[VMEM, SMEM] + [VMEM] * 7,
        out_specs=(VMEM,) * 3,
        out_shape=shapes(((32, 2048), F32), ((8, 128), F32), ((8, 12, 32), F32)),
        scratch_shapes=[pltpu.VMEM((144, 2048), BF), pltpu.VMEM((216, 2048), F32)],
        name="mid",
    )(slots, where, a_mid, bu_mid, *mid)
    latent_mid = lax.all_to_all(latent, "chan", 0, 0, tiled=True)
    latent_top, loglik = pl.pallas_call(
        top_kernel,
        in_specs=[VMEM, VMEM, SMEM] + [VMEM] * 14,
        out_specs=(VMEM,) * 2,
        out_shape=shapes(((48, 64), F32), ((8, 128), F32)),
        scratch_shapes=[
            pltpu.VMEM((144, 2048), BF), pltpu.VMEM((216, 2048), F32), pltpu.VMEM((224, 512), BF), pltpu.VMEM((432, 512), F32),
        ],
        name="top",
    )(u, sums, where, const, *mid, *top)
    return latent_mid.reshape(8, 12, 1, 32), latent_top.reshape(1, 48, 4, 16), loglik[0, :1]


def solution(mesh):
    return jax.shard_map(
        body,
        mesh=mesh,
        in_specs=(P("batch", None, ("rows", "chan"), None),) + (P(),) * 22,
        out_specs=(
            P("batch", None, ("rows", "chan"), None),
            P(("batch", "chan"), None, "rows", None),
            P(("batch", "chan")),
        ),
        check_vma=False,
    )
```

```python
import functools
import math

import jax
import jax.numpy as jnp
from jax import lax
from jax.experimental import pallas as pl
from jax.experimental.pallas import tpu as pltpu
from jax.sharding import PartitionSpec as P

BF = jnp.bfloat16
F32 = jnp.float32
log_two_pi = math.log(2.0 * math.pi)
VMEM = pl.BlockSpec(memory_space=pltpu.VMEM)
SMEM = pl.BlockSpec(memory_space=pltpu.SMEM)
HBM = pl.BlockSpec(memory_space=pltpu.HBM)


def iota(shape, dim):
    return lax.broadcasted_iota(jnp.int32, shape, dim)


def eye(n, dtype):
    return (iota((n, n), 0) == iota((n, n), 1)).astype(dtype)


def dot_t(a, b):
    return lax.dot_general(a, b, (((1,), (1,)), ((), ())), preferred_element_type=F32)


def dot(a, b):
    return jnp.dot(a, b, preferred_element_type=F32)


def halves(x):
    high = x.astype(BF)
    return high, (x - high.astype(F32)).astype(BF)


def to_column(row):
    n = row.shape[1]
    same = iota((n, n), 0) == iota((n, n), 1)
    return jnp.sum(jnp.where(same, row, 0.0), axis=1, keepdims=True)


def three_term_left(matrix):
    high, low = halves(matrix)
    return jnp.concatenate([high, high, low], axis=1)


def select_rows(n_out, n_in, source_of):
    return (iota((n_out, n_in), 1) == source_of(iota((n_out, n_in), 0))).astype(F32)


def spread_mid(o):
    return jnp.where(o < 12, o, jnp.where(o >= 20, o - 8, -1))


def flow_matrix(gain, lower, upper, diag, shift, n):
    i, j = iota((n, n), 0), iota((n, n), 1)
    low = jnp.where(i > j, lower, 0.0) + jnp.where(i == j, 1.0, 0.0)
    up = jnp.where(i < j, upper, 0.0) + jnp.where(i == j, jnp.exp(diag), 0.0)
    matrix = jnp.dot(low, up, precision=lax.Precision.HIGHEST, preferred_element_type=F32)
    matrix = matrix * jnp.exp(gain)
    return matrix, jnp.sum(matrix * shift, axis=1, keepdims=True)


def exact_dot(a, b):
    return jnp.dot(a, b, precision=lax.Precision.HIGHEST, preferred_element_type=F32)


def prep_kernel(
    shift_mid, gain_mid, lower_mid, upper_mid, diag_mid, first_mid, first_bias_mid, second_mid,
    second_bias_mid, third_bias_mid,
    shift_top, gain_top, lower_top, upper_top, diag_top, first_top, first_bias_top, second_top,
    second_bias_top, third_bias_top,
    a_mid, bu_mid, w1_mid, w2_mid, b2_mid, b3_mid,
    a_top0, a_top1, bu_top, w1_top, w2_top, b2_top, b3_top, const,
):
    hid = second_mid.shape[1]
    ident = eye(hid, BF)
    total = jnp.zeros((1, 1), F32)
    for s in range(3):
        row = slice(s, s + 1)
        matrix, offset = flow_matrix(gain_mid[row], lower_mid[s], upper_mid[s], diag_mid[row], shift_mid[row], 24)
        total = total + 2048.0 * jnp.sum(gain_mid[row] + diag_mid[row], axis=1, keepdims=True)
        rows = select_rows(32, 24, spread_mid)
        matrix = exact_dot(rows, matrix)
        offset = jnp.sum(rows * jnp.sum(jnp.where(eye(24, F32) > 0, offset, 0.0), axis=0, keepdims=True), axis=1, keepdims=True)
        offset = offset + (iota((32, 1), 0) == 12).astype(F32)
        if s == 0:
            columns = (iota((24, 32), 0) == iota((24, 32), 1)).astype(F32)
        else:
            columns = (iota((24, 32), 0) == spread_mid(iota((24, 32), 1))).astype(F32)
        a_mid[s] = three_term_left(exact_dot(matrix, columns))
        bu_mid[s] = jnp.broadcast_to(offset, (32, 128))
        zeros = jnp.zeros((4, hid), F32)
        with_bias = jnp.concatenate([first_bias_mid[row].astype(F32), zeros[:3]], axis=0)
        blocks = []
        for tap in range(9):
            blocks += [first_mid[s, tap].astype(F32), with_bias if tap == 4 else zeros]
        w1_mid[s] = dot_t(ident, jnp.concatenate(blocks, axis=0).astype(BF)).astype(BF)
        w2_mid[s] = dot_t(ident, second_mid[s]).astype(BF)
        b2_mid[s] = jnp.broadcast_to(second_bias_mid[row], (8, hid))
        b3 = to_column(third_bias_mid[row]) + jnp.where(iota((24, 1), 0) < 12, 2.0, 0.0)
        b3_mid[s] = jnp.broadcast_to(b3, (24, 128))
    for s in range(2):
        row = slice(s, s + 1)
        matrix, offset = flow_matrix(gain_top[row], lower_top[s], upper_top[s], diag_top[row], shift_top[row], 48)
        total = total + 512.0 * jnp.sum(gain_top[row] + diag_top[row], axis=1, keepdims=True)
        if s == 0:
            k = iota((48, 64), 1)
            source = jnp.where(k % 16 >= 4, 4 * (k % 16 - 4) + k // 16, -1)
            a_top0[...] = three_term_left(exact_dot(matrix, (iota((48, 64), 0) == source).astype(F32)))
        else:
            a_top1[...] = three_term_left(matrix)
        bu_top[s] = jnp.broadcast_to(offset, (48, 128))
        blocks = [first_top[s, tap].astype(F32) for tap in range(9)]
        blocks += [first_bias_top[row].astype(F32), jnp.zeros((7, hid), F32)]
        w1_top[s] = dot_t(ident, jnp.concatenate(blocks, axis=0).astype(BF)).astype(BF)
        w2_top[s] = dot_t(ident, second_top[s]).astype(BF)
        b2_top[s] = jnp.broadcast_to(second_bias_top[row], (128, hid)).T
        b3 = to_column(third_bias_top[row]) + jnp.where(iota((48, 1), 0) < 24, 2.0, 0.0)
        b3_top[s] = jnp.broadcast_to(b3, (48, 128))
    const[...] = jnp.broadcast_to(total, (8, 128))


def tiled(column, lanes):
    return jnp.concatenate([column] * (lanes // 128), axis=1)


def moved(x, by):
    lanes = x.shape[1]
    return pltpu.roll(x, (-by) % lanes, 1)


def row_moved(x, dr, width):
    if dr == 0:
        return x
    lane = iota(x.shape, 1)
    inside = lane >= width if dr < 0 else lane < x.shape[1] - width
    return jnp.where(inside, moved(x, dr * width), 0.0)


def column_moved(x, dc, width):
    if dc == 0:
        return x
    column = iota(x.shape, 1) % width
    inside = column >= 1 if dc < 0 else column <= width - 2
    return jnp.where(inside, moved(x, dc), 0.0)


def conditioner(q, extra, refs, copies, x_scr, p_scr, width, chunk):
    cells = q.shape[1]
    rows = q.shape[0]
    sides = [column_moved(q, dc, width) for dc in (-1, 0, 1)]
    blocks = [row_moved(side, dr, width) for dr in (-1, 0, 1) for side in sides]
    if extra is not None:
        blocks.append(extra)
    x_scr[...] = jnp.concatenate(blocks, axis=0).astype(BF)
    if len(copies) > 1:
        awaited(copies)
    w1_ref, w2_ref, b2_ref, w3_ref, b3_ref = refs
    w1, w2, b3 = w1_ref[...], w2_ref[...], b3_ref[...]
    b2 = b2_ref[...]
    if b2.shape[0] == 8:
        b2 = jnp.concatenate([b2] * 16, axis=0).T
    bias = tiled(b2, chunk)

    def one(i):
        at = pl.ds(i * chunk, chunk)
        inner = jnp.maximum(dot(w1, x_scr[:, at]), 0.0).astype(BF)
        middle = jnp.maximum(dot(w2, inner) + bias, 0.0).astype(BF)
        if i == 0 and len(copies) == 1:
            awaited(copies)
        p_scr[:, at] = dot(w3_ref[...], middle)

    for i in range(cells // chunk):
        one(i)
    n_out = p_scr.shape[0] // 9
    out = tiled(b3, cells)
    for dc in (-1, 0, 1):
        part = None
        for dr in (-1, 0, 1):
            tap = 3 * (dr + 1) + dc + 1
            term = row_moved(p_scr[n_out * tap : n_out * (tap + 1), :], dr, width)
            part = term if part is None else part + term
        out = out + column_moved(part, dc, width)
    return out


def gate_of(g):
    e = jnp.exp(-jnp.abs(g))
    scale = 1.0 / (1.0 + e)
    return jnp.where(g >= 0.0, scale, e * scale), jnp.minimum(g, 0.0) - jnp.log(1.0 + e)


def mix(a, parts, bias):
    return dot(a, jnp.concatenate(parts, axis=0)) + bias


def mid_update(u, refs, copies, x_scr, p_scr):
    out = conditioner(u[:16], None, refs, copies, x_scr, p_scr, 32, 1024)
    scale, logs = gate_of(out[:16])
    logs = jnp.where(iota(logs.shape, 0) < 12, logs, 0.0)
    updated = (u[16:] + out[8:]) * pltpu.roll(scale, 4, 0)
    return updated, jnp.sum(logs, keepdims=True)


def started(pairs, sems):
    copies = [pltpu.make_async_copy(a, b, sems.at[k]) for k, (a, b) in enumerate(pairs)]
    for copy in copies:
        copy.start()
    return copies


def awaited(copies):
    for copy in copies:
        copy.wait()


def mid_kernel(where, slots, a_mid, bu_mid, b3, w1, w2, b2, w3h, u_out, sum_out, latent_out, x_scr, p_scr, w3, sems):
    copies = started([(w3h.at[s], w3.at[s]) for s in range(2)], sems)
    cells = 2048
    lane = iota((8, 128), 1) // 32
    groups = []
    for g in range(3):
        pieces = []
        for k in range(16):
            piece = None
            for j in range(4):
                source = slots[4 * k + j]
                turn = (32 * (j - g)) % 128
                source = pltpu.roll(source, turn, 1) if turn else source
                piece = source if piece is None else jnp.where(lane == j, source, piece)
            pieces.append(piece)
        groups.append(jnp.concatenate(pieces, axis=1))
    state = jnp.concatenate(groups + [jnp.zeros((8, cells), F32)], axis=0)
    total = jnp.zeros((1, 1), F32)
    for s in range(2):
        high, low = halves(state)
        u = mix(a_mid[s], [high, low, high], tiled(bu_mid[s], cells))
        updated, logs = mid_update(u, (w1.at[s], w2.at[s], b2.at[s], w3.at[s], b3.at[s]), copies[s : s + 1], x_scr, p_scr)
        total = total + logs
        state = jnp.concatenate([u[:16], updated], axis=0)
    high, low = halves(state)
    u = mix(a_mid[2], [high, low, high], tiled(bu_mid[2], cells))
    u_out[...] = u
    latent = jnp.where(iota((16, cells), 0) < 12, u[:16], 0.0)
    total = total - 0.5 * jnp.sum(latent * latent, keepdims=True)
    sum_out[...] = jnp.broadcast_to(total, (8, 128))
    own = u_out[0:16, pl.ds(pl.multiple_of(where[0] * 256, 256), 256)]
    for j in range(8):
        part = own[:, 128 * (j // 4) : 128 * (j // 4) + 128]
        latent_out[j] = pltpu.roll(part, 128 - 32 * (j % 4), 1) if j % 4 else part


def top_kernel(where, u_in, sum_in, b3m, w1m, w2m, b2m, w3mh, w1h, w2h, b2h, w3h, *rest):
    small_h, (latent_out, sum_out, x_scr, p_scr, xt_scr, pt_scr, w3m, w1, w2, b2, w3, *small, sems) = rest[:5], rest[5:]
    a_top0, a_top1, bu_top, b3, const = small
    pairs = [(w3mh.at[2], w3m)] + list(zip(small_h, small))
    for s in range(2):
        pairs += [(a.at[s], b.at[s]) for a, b in zip((w1h, w2h, b2h, w3h), (w1, w2, b2, w3))]
    copies = started(pairs, sems)
    refs = (w1m.at[2], w2m.at[2], b2m.at[2], w3m, b3m.at[2])
    updated, logs = mid_update(u_in[...], refs, copies[:1], x_scr, p_scr)
    awaited(copies[1:6])
    total = sum_in[0:1, 0:1] + const[0:1, 0:1] + logs
    high, low = halves(updated)
    cell = iota((128, 128), 0)
    target = 32 * (2 * (cell // 32 % 2) + cell % 2) + 16 * (cell // 64) + cell % 32 // 2
    order = (target == iota((128, 128), 1)).astype(BF)
    stacked = jnp.concatenate([part[:, 128 * k : 128 * k + 128] for part in (high, low) for k in range(16)], axis=0)
    stacked = dot(stacked, order)
    lane = iota((16, 128), 1) // 32
    parts = []
    for p in range(2):
        for ij in range(4):
            pieces = []
            for m in range(4):
                piece = None
                for j in range(4):
                    start = 256 * p + 16 * (4 * m + j)
                    source = stacked[start : start + 16]
                    turn = (32 * (j - ij)) % 128
                    source = pltpu.roll(source, turn, 1) if turn else source
                    piece = source if piece is None else jnp.where(lane == j, source, piece)
                pieces.append(piece)
            parts.append(jnp.concatenate(pieces, axis=1).astype(BF))
    u = mix(a_top0[...], parts + parts[:4], tiled(bu_top[0], 512))
    ones = (iota((8, 512), 0) == 0).astype(F32)
    for s in range(2):
        out = conditioner(u[:24], ones, (w1.at[s], w2.at[s], b2.at[s], w3.at[s], b3.at[s]), copies[6 + 4 * s : 10 + 4 * s], xt_scr, pt_scr, 16, 512)
        scale, logs = gate_of(out[:24])
        total = total + jnp.sum(logs, keepdims=True)
        state = jnp.concatenate([u[:24], (u[24:] + out[24:]) * scale], axis=0)
        if s == 0:
            high, low = halves(state)
            u = mix(a_top1[...], [high, low, high], tiled(bu_top[1], 512))
    total = total - 0.5 * jnp.sum(state * state, keepdims=True)
    total = (total - 0.5 * log_two_pi * 49152.0) * (1.0 / 49152.0)
    sum_out[0] = total[0, 0]
    block = pltpu.roll(state, (512 - where[0] * 64) % 512, 1)
    block = jnp.concatenate([block[:, :128], jnp.zeros((80, 128), F32)], axis=0)
    latent_out[...] = block.T[:64, :48]


def pack_kernel(images, packed):
    for i in range(8):
        rows = images[i]
        wide = jnp.concatenate([rows[0:8], rows[8:16], rows[16:24], jnp.zeros((8, 32), F32)], axis=1)
        for r in range(8):
            packed[8 * r + i] = wide


def shapes(*items):
    return tuple(jax.ShapeDtypeStruct(shape, dtype) for shape, dtype in items)


def in_vmem(x):
    return pltpu.with_memory_space_constraint(x, pltpu.VMEM)


def in_hbm(x):
    return pltpu.with_memory_space_constraint(x, pltpu.HBM)


def call(kernel, name, inputs, specs, outputs, scratch=(), out_specs=None, limit=None):
    return pl.pallas_call(
        kernel,
        in_specs=specs,
        out_specs=out_specs or (VMEM,) * len(outputs),
        out_shape=tuple(outputs),
        scratch_shapes=list(scratch),
        compiler_params=pltpu.CompilerParams(vmem_limit_bytes=limit),
        name=name,
    )(*inputs)


def pack(images):
    return pl.pallas_call(
        pack_kernel, in_specs=[VMEM], out_specs=VMEM, out_shape=jax.ShapeDtypeStruct((64, 8, 128), F32), name="pack"
    )(images.reshape(8, 24, 32))


def prep(params):
    small = [p for i, p in enumerate(params) if i not in (9, 20)]
    return call(
        prep_kernel,
        "prep",
        small,
        [VMEM] * 20,
        (
            pltpu.VMEM((3, 32, 96), BF), pltpu.VMEM((3, 32, 128), F32), pltpu.VMEM((3, 512, 144), BF), pltpu.VMEM((3, 512, 512), BF),
            pltpu.VMEM((3, 8, 512), F32), pltpu.VMEM((3, 24, 128), F32),
        )
        + shapes(
            ((48, 192), BF), ((48, 144), BF), ((2, 48, 128), F32), ((2, 512, 224), BF), ((2, 512, 512), BF), ((2, 512, 128), F32),
            ((2, 48, 128), F32), ((8, 128), F32),
        ),
    )


MID_SCRATCH = (pltpu.VMEM((144, 2048), BF), pltpu.VMEM((216, 2048), F32))


def mid(where, slots, prepared, third):
    a, bu, w1, w2, b2, b3 = (in_vmem(x) for x in prepared[:6])
    return call(
        mid_kernel,
        "mid",
        [where, in_vmem(slots), a, bu, b3, w1, w2, b2, in_hbm(third)],
        [SMEM] + [VMEM] * 7 + [HBM],
        [pltpu.VMEM((32, 2048), F32), pltpu.VMEM((8, 128), F32), jax.ShapeDtypeStruct((8, 16, 128), F32)],
        MID_SCRATCH + (pltpu.VMEM((2, 216, 512), BF), pltpu.SemaphoreType.DMA((2,))),
        limit=24 * 2**20,
    )


def top(where, u, sums, prepared, third_m, third):
    w1m, w2m, b2m, b3m = (in_vmem(x) for x in prepared[2:6])
    a0, a1, bu, w1, w2, b2, b3, const = prepared[6:]
    return call(
        top_kernel,
        "top",
        [where, in_vmem(u), in_vmem(sums), b3m, w1m, w2m, b2m]
        + [in_hbm(x) for x in (third_m, w1, w2, b2, third, a0, a1, bu, b3, const)],
        [SMEM] + [VMEM] * 6 + [HBM] * 10,
        [jax.ShapeDtypeStruct((64, 48), F32), jax.ShapeDtypeStruct((1,), F32)],
        MID_SCRATCH
        + (
            pltpu.VMEM((224, 512), BF), pltpu.VMEM((432, 512), F32), pltpu.VMEM((216, 512), BF),
            pltpu.VMEM((2, 512, 224), BF), pltpu.VMEM((2, 512, 512), BF), pltpu.VMEM((2, 512, 128), F32), pltpu.VMEM((2, 432, 512), BF),
            pltpu.VMEM((48, 192), BF), pltpu.VMEM((48, 144), BF), pltpu.VMEM((2, 48, 128), F32), pltpu.VMEM((2, 48, 128), F32), pltpu.VMEM((8, 128), F32),
            pltpu.SemaphoreType.DMA((14,)),
        ),
        (VMEM, SMEM),
        limit=24 * 2**20,
    )


def body(images, *params):
    slots = lax.all_to_all(pack(images), ("rows", "chan"), 0, 0, tiled=True)
    third_mid = params[9].transpose(0, 1, 3, 2).reshape(3, 216, 512)
    third_top = params[20].transpose(0, 1, 3, 2).reshape(2, 432, 512)
    prepared = prep(params)
    where = lax.axis_index("rows").astype(jnp.int32).reshape(1)
    u, sums, latent = mid(where, slots, prepared, third_mid)
    latent_mid = lax.all_to_all(latent, "chan", 0, 0, tiled=True)
    latent_top, loglik = top(where, u, sums, prepared, third_mid, third_top)
    latent_top = latent_top.reshape(1, 4, 16, 48).transpose(0, 3, 1, 2)
    return latent_mid[:, :12, None, :32], latent_top, loglik


def solution(mesh):
    return jax.shard_map(
        body,
        mesh=mesh,
        in_specs=(P("batch", None, ("rows", "chan"), None),) + (P(),) * 22,
        out_specs=(
            P("batch", None, ("rows", "chan"), None),
            P(("batch", "chan"), None, "rows", None),
            P(("batch", "chan")),
        ),
        check_vma=False,
    )
```

```python
import functools
import math

import jax
import jax.numpy as jnp
from jax import lax
from jax.experimental import pallas as pl
from jax.experimental.pallas import tpu as pltpu
from jax.sharding import PartitionSpec as P

BF = jnp.bfloat16
F32 = jnp.float32
log_two_pi = math.log(2.0 * math.pi)
VMEM = pl.BlockSpec(memory_space=pltpu.VMEM)
SMEM = pl.BlockSpec(memory_space=pltpu.SMEM)
HBM = pl.BlockSpec(memory_space=pltpu.HBM)


def iota(shape, dim):
    return lax.broadcasted_iota(jnp.int32, shape, dim)


def eye(n, dtype):
    return (iota((n, n), 0) == iota((n, n), 1)).astype(dtype)


def dot_t(a, b):
    return lax.dot_general(a, b, (((1,), (1,)), ((), ())), preferred_element_type=F32)


def dot(a, b):
    return jnp.dot(a, b, preferred_element_type=F32)


def halves(x):
    high = x.astype(BF)
    return high, (x - high.astype(F32)).astype(BF)


def to_column(row):
    n = row.shape[1]
    same = iota((n, n), 0) == iota((n, n), 1)
    return jnp.sum(jnp.where(same, row, 0.0), axis=1, keepdims=True)


def three_term_left(matrix):
    high, low = halves(matrix)
    return jnp.concatenate([high, high, low], axis=1)


def select_rows(n_out, n_in, source_of):
    return (iota((n_out, n_in), 1) == source_of(iota((n_out, n_in), 0))).astype(F32)


def spread_mid(o):
    return jnp.where(o < 12, o, jnp.where(o >= 20, o - 8, -1))


def flow_matrix(gain, lower, upper, diag, shift, n):
    i, j = iota((n, n), 0), iota((n, n), 1)
    low = jnp.where(i > j, lower, 0.0) + jnp.where(i == j, 1.0, 0.0)
    up = jnp.where(i < j, upper, 0.0) + jnp.where(i == j, jnp.exp(diag), 0.0)
    matrix = jnp.dot(low, up, precision=lax.Precision.HIGHEST, preferred_element_type=F32)
    matrix = matrix * jnp.exp(gain)
    return matrix, jnp.sum(matrix * shift, axis=1, keepdims=True)


def exact_dot(a, b):
    return jnp.dot(a, b, precision=lax.Precision.HIGHEST, preferred_element_type=F32)


def prep_kernel(
    shift_mid, gain_mid, lower_mid, upper_mid, diag_mid, first_mid, first_bias_mid, second_mid,
    second_bias_mid, third_bias_mid,
    shift_top, gain_top, lower_top, upper_top, diag_top, first_top, first_bias_top, second_top,
    second_bias_top, third_bias_top,
    a_mid, bu_mid, w1_mid, w2_mid, b2_mid, b3_mid,
    a_top0, a_top1, bu_top, w1_top, w2_top, b2_top, b3_top, const,
):
    hid = second_mid.shape[1]
    ident = eye(hid, BF)
    total = jnp.zeros((1, 1), F32)
    for s in range(3):
        row = slice(s, s + 1)
        matrix, offset = flow_matrix(gain_mid[row], lower_mid[s], upper_mid[s], diag_mid[row], shift_mid[row], 24)
        total = total + 2048.0 * jnp.sum(gain_mid[row] + diag_mid[row], axis=1, keepdims=True)
        rows = select_rows(32, 24, spread_mid)
        matrix = exact_dot(rows, matrix)
        offset = jnp.sum(rows * jnp.sum(jnp.where(eye(24, F32) > 0, offset, 0.0), axis=0, keepdims=True), axis=1, keepdims=True)
        offset = offset + (iota((32, 1), 0) == 12).astype(F32)
        if s == 0:
            held = iota((24, 32), 1)
            columns = (iota((24, 32), 0) == jnp.where(held % 8 < 6, held // 8 * 6 + held % 8, -1)).astype(F32)
        else:
            columns = (iota((24, 32), 0) == spread_mid(iota((24, 32), 1))).astype(F32)
        a_mid[s] = three_term_left(exact_dot(matrix, columns))
        bu_mid[s] = jnp.broadcast_to(offset, (32, 128))
        zeros = jnp.zeros((4, hid), F32)
        with_bias = jnp.concatenate([first_bias_mid[row].astype(F32), zeros[:3]], axis=0)
        blocks = []
        for tap in range(9):
            blocks += [first_mid[s, tap].astype(F32), with_bias if tap == 4 else zeros]
        w1_mid[s] = dot_t(ident, jnp.concatenate(blocks, axis=0).astype(BF)).astype(BF)
        w2_mid[s] = dot_t(ident, second_mid[s]).astype(BF)
        b2_mid[s] = jnp.broadcast_to(second_bias_mid[row], (8, hid))
        b3 = to_column(third_bias_mid[row]) + jnp.where(iota((24, 1), 0) < 12, 2.0, 0.0)
        b3_mid[s] = jnp.broadcast_to(b3, (24, 128))
    for s in range(2):
        row = slice(s, s + 1)
        matrix, offset = flow_matrix(gain_top[row], lower_top[s], upper_top[s], diag_top[row], shift_top[row], 48)
        total = total + 512.0 * jnp.sum(gain_top[row] + diag_top[row], axis=1, keepdims=True)
        if s == 0:
            k = iota((48, 64), 1)
            source = jnp.where(k % 16 >= 4, 4 * (k % 16 - 4) + k // 16, -1)
            a_top0[...] = three_term_left(exact_dot(matrix, (iota((48, 64), 0) == source).astype(F32)))
        else:
            a_top1[...] = three_term_left(matrix)
        bu_top[s] = jnp.broadcast_to(offset, (48, 128))
        blocks = [first_top[s, tap].astype(F32) for tap in range(9)]
        blocks += [first_bias_top[row].astype(F32), jnp.zeros((7, hid), F32)]
        w1_top[s] = dot_t(ident, jnp.concatenate(blocks, axis=0).astype(BF)).astype(BF)
        w2_top[s] = dot_t(ident, second_top[s]).astype(BF)
        b2_top[s] = jnp.broadcast_to(second_bias_top[row], (128, hid)).T
        b3 = to_column(third_bias_top[row]) + jnp.where(iota((48, 1), 0) < 24, 2.0, 0.0)
        b3_top[s] = jnp.broadcast_to(b3, (48, 128))
    const[...] = jnp.broadcast_to(total, (8, 128))


def tiled(column, lanes):
    return jnp.concatenate([column] * (lanes // 128), axis=1)


def moved(x, by):
    lanes = x.shape[1]
    return pltpu.roll(x, (-by) % lanes, 1)


def row_moved(x, dr, width):
    if dr == 0:
        return x
    lane = iota(x.shape, 1)
    inside = lane >= width if dr < 0 else lane < x.shape[1] - width
    return jnp.where(inside, moved(x, dr * width), 0.0)


def column_moved(x, dc, width):
    if dc == 0:
        return x
    column = iota(x.shape, 1) % width
    inside = column >= 1 if dc < 0 else column <= width - 2
    return jnp.where(inside, moved(x, dc), 0.0)


def conditioner(q, extra, refs, copies, x_scr, p_scr, width, chunk):
    cells = q.shape[1]
    rows = q.shape[0]
    sides = [column_moved(q, dc, width) for dc in (-1, 0, 1)]
    blocks = [row_moved(side, dr, width) for dr in (-1, 0, 1) for side in sides]
    if extra is not None:
        blocks.append(extra)
    x = jnp.concatenate(blocks, axis=0).astype(BF)
    outs = []
    if len(copies) > 1:
        awaited(copies)
    w1_ref, w2_ref, b2_ref, w3_ref, b3_ref = refs
    w1, w2, b3 = w1_ref[...], w2_ref[...], b3_ref[...]
    b2 = b2_ref[...]
    if b2.shape[0] == 8:
        b2 = jnp.concatenate([b2] * 16, axis=0).T
    bias = tiled(b2, chunk)

    n = cells // chunk
    inner = [jnp.maximum(dot(w1, x[:, i * chunk : (i + 1) * chunk]), 0.0).astype(BF) for i in range(n)]
    middle = [jnp.maximum(dot(w2, y) + bias, 0.0).astype(BF) for y in inner]
    if len(copies) == 1:
        awaited(copies)
    outs = [dot(w3_ref[...], y) for y in middle]
    p = outs[0] if len(outs) == 1 else jnp.concatenate(outs, axis=1)
    n_out = p.shape[0] // 9
    out = tiled(b3, cells)
    for dc in (-1, 0, 1):
        part = None
        for dr in (-1, 0, 1):
            tap = 3 * (dr + 1) + dc + 1
            term = row_moved(p[n_out * tap : n_out * (tap + 1), :], dr, width)
            part = term if part is None else part + term
        out = out + column_moved(part, dc, width)
    return out


def gate_of(g):
    e = jnp.exp(-jnp.abs(g))
    scale = 1.0 / (1.0 + e)
    return jnp.where(g >= 0.0, scale, e * scale), jnp.minimum(g, 0.0) - jnp.log(1.0 + e)


def mix(a, parts, bias):
    return dot(a, jnp.concatenate(parts, axis=0)) + bias


def mid_update(u, refs, copies, x_scr, p_scr, chunk=1024):
    out = conditioner(u[:16], None, refs, copies, x_scr, p_scr, 32, chunk)
    scale, logs = gate_of(out[:16])
    logs = jnp.where(iota(logs.shape, 0) < 12, logs, 0.0)
    updated = (u[16:] + out[8:]) * pltpu.roll(scale, 4, 0)
    return updated, jnp.sum(logs, keepdims=True)


def started(pairs, sems):
    copies = [pltpu.make_async_copy(a, b, sems.at[k]) for k, (a, b) in enumerate(pairs)]
    for copy in copies:
        copy.start()
    return copies


def awaited(copies):
    for copy in copies:
        copy.wait()


def mid_kernel(where, slots, a_mid, bu_mid, b3, w1, w2, b2, w3h, u_out, sum_out, latent_out, x_scr, p_scr, w3, sems):
    copies = started([(w3h.at[s], w3.at[s]) for s in range(2)], sems)
    cells = 2048
    lane = iota((8, 128), 1) // 32
    groups = []
    for g in range(4):
        pieces = []
        for k in range(16):
            piece = None
            for j in range(4):
                source = jnp.concatenate([slots[4 * k + j, t] for t in range(3)] + [jnp.zeros((2, 128), F32)], axis=0)
                turn = (32 * (j - g)) % 128
                source = pltpu.roll(source, turn, 1) if turn else source
                piece = source if piece is None else jnp.where(lane == j, source, piece)
            pieces.append(piece)
        groups.append(jnp.concatenate(pieces, axis=1))
    state = jnp.concatenate(groups, axis=0)
    total = jnp.zeros((1, 1), F32)
    for s in range(2):
        high, low = halves(state)
        u = mix(a_mid[s], [high, low, high], tiled(bu_mid[s], cells))
        updated, logs = mid_update(u, (w1.at[s], w2.at[s], b2.at[s], w3.at[s], b3.at[s]), copies[s : s + 1], x_scr, p_scr)
        total = total + logs
        state = jnp.concatenate([u[:16], updated], axis=0)
    high, low = halves(state)
    u = mix(a_mid[2], [high, low, high], tiled(bu_mid[2], cells))
    u_out[...] = u
    latent = jnp.where(iota((16, cells), 0) < 12, u[:16], 0.0)
    total = total - 0.5 * jnp.sum(latent * latent, keepdims=True)
    sum_out[...] = jnp.broadcast_to(total, (8, 128))
    own = u_out[0:16, pl.ds(pl.multiple_of(where[0] * 256, 256), 256)]
    for j in range(8):
        part = own[:, 128 * (j // 4) : 128 * (j // 4) + 128]
        latent_out[j] = pltpu.roll(part, 128 - 32 * (j % 4), 1) if j % 4 else part


def top_kernel(where, u_in, sum_in, b3m, w1m, w2m, b2m, w3mh, w1h, w2h, b2h, w3h, *rest):
    small_h, (latent_out, sum_out, x_scr, p_scr, xt_scr, pt_scr, w3m, w1, w2, b2, w3, *small, sems) = rest[:5], rest[5:]
    a_top0, a_top1, bu_top, b3, const = small
    pairs = [(w3mh.at[2], w3m)] + list(zip(small_h, small))
    for s in range(2):
        pairs += [(a.at[s], b.at[s]) for a, b in zip((w1h, w2h, b2h, w3h), (w1, w2, b2, w3))]
    copies = started(pairs, sems)
    refs = (w1m.at[2], w2m.at[2], b2m.at[2], w3m, b3m.at[2])
    updated, logs = mid_update(u_in[...], refs, copies[:1], x_scr, p_scr, 2048)
    awaited(copies[1:6])
    total = sum_in[0:1, 0:1] + const[0:1, 0:1] + logs
    high, low = halves(updated)
    cell = iota((128, 128), 0)
    target = 32 * (2 * (cell // 32 % 2) + cell % 2) + 16 * (cell // 64) + cell % 32 // 2
    order = (target == iota((128, 128), 1)).astype(BF)
    stacked = jnp.concatenate([part[:, 128 * k : 128 * k + 128] for part in (high, low) for k in range(16)], axis=0)
    stacked = dot(stacked, order)
    lane = iota((16, 128), 1) // 32
    parts = []
    for p in range(2):
        for ij in range(4):
            pieces = []
            for m in range(4):
                piece = None
                for j in range(4):
                    start = 256 * p + 16 * (4 * m + j)
                    source = stacked[start : start + 16]
                    turn = (32 * (j - ij)) % 128
                    source = pltpu.roll(source, turn, 1) if turn else source
                    piece = source if piece is None else jnp.where(lane == j, source, piece)
                pieces.append(piece)
            parts.append(jnp.concatenate(pieces, axis=1).astype(BF))
    u = mix(a_top0[...], parts + parts[:4], tiled(bu_top[0], 512))
    ones = (iota((8, 512), 0) == 0).astype(F32)
    for s in range(2):
        out = conditioner(u[:24], ones, (w1.at[s], w2.at[s], b2.at[s], w3.at[s], b3.at[s]), copies[6 + 4 * s : 10 + 4 * s], xt_scr, pt_scr, 16, 512)
        scale, logs = gate_of(out[:24])
        total = total + jnp.sum(logs, keepdims=True)
        state = jnp.concatenate([u[:24], (u[24:] + out[24:]) * scale], axis=0)
        if s == 0:
            high, low = halves(state)
            u = mix(a_top1[...], [high, low, high], tiled(bu_top[1], 512))
    total = total - 0.5 * jnp.sum(state * state, keepdims=True)
    total = (total - 0.5 * log_two_pi * 49152.0) * (1.0 / 49152.0)
    sum_out[0] = total[0, 0]
    block = pltpu.roll(state, (512 - where[0] * 64) % 512, 1)
    block = jnp.concatenate([block[:, :128], jnp.zeros((80, 128), F32)], axis=0)
    latent_out[...] = block.T[:64, :48]


def pack_kernel(images, packed):
    for i in range(8):
        rows = images[i]
        wide = jnp.concatenate([rows[6 * j : 6 * j + 6] for j in range(4)], axis=1)
        for r in range(8):
            for t in range(3):
                packed[8 * r + i, t] = wide[2 * t : 2 * t + 2]


def shapes(*items):
    return tuple(jax.ShapeDtypeStruct(shape, dtype) for shape, dtype in items)


def in_vmem(x):
    return pltpu.with_memory_space_constraint(x, pltpu.VMEM)


def in_hbm(x):
    return pltpu.with_memory_space_constraint(x, pltpu.HBM)


def call(kernel, name, inputs, specs, outputs, scratch=(), out_specs=None, limit=None):
    return pl.pallas_call(
        kernel,
        in_specs=specs,
        out_specs=out_specs or (VMEM,) * len(outputs),
        out_shape=tuple(outputs),
        scratch_shapes=list(scratch),
        compiler_params=pltpu.CompilerParams(vmem_limit_bytes=limit),
        name=name,
    )(*inputs)


def pack(images):
    return pl.pallas_call(
        pack_kernel, in_specs=[VMEM], out_specs=VMEM, out_shape=jax.ShapeDtypeStruct((64, 3, 2, 128), F32), name="pack"
    )(images.reshape(8, 24, 32))


def prep(params):
    small = [p for i, p in enumerate(params) if i not in (9, 20)]
    return call(
        prep_kernel,
        "prep",
        small,
        [VMEM] * 20,
        (
            pltpu.VMEM((3, 32, 96), BF), pltpu.VMEM((3, 32, 128), F32), pltpu.VMEM((3, 512, 144), BF), pltpu.VMEM((3, 512, 512), BF),
            pltpu.VMEM((3, 8, 512), F32), pltpu.VMEM((3, 24, 128), F32),
        )
        + shapes(
            ((48, 192), BF), ((48, 144), BF), ((2, 48, 128), F32), ((2, 512, 224), BF), ((2, 512, 512), BF), ((2, 512, 128), F32),
            ((2, 48, 128), F32), ((8, 128), F32),
        ),
    )


MID_SCRATCH = (pltpu.VMEM((144, 2048), BF), pltpu.VMEM((216, 2048), F32))


def mid(where, slots, prepared, third):
    a, bu, w1, w2, b2, b3 = (in_vmem(x) for x in prepared[:6])
    return call(
        mid_kernel,
        "mid",
        [where, in_vmem(slots), a, bu, b3, w1, w2, b2, in_hbm(third)],
        [SMEM] + [VMEM] * 7 + [HBM],
        [pltpu.VMEM((32, 2048), F32), pltpu.VMEM((8, 128), F32), jax.ShapeDtypeStruct((8, 16, 128), F32)],
        MID_SCRATCH + (pltpu.VMEM((2, 216, 512), BF), pltpu.SemaphoreType.DMA((2,))),
        limit=24 * 2**20,
    )


def top(where, u, sums, prepared, third_m, third):
    w1m, w2m, b2m, b3m = (in_vmem(x) for x in prepared[2:6])
    a0, a1, bu, w1, w2, b2, b3, const = prepared[6:]
    return call(
        top_kernel,
        "top",
        [where, in_vmem(u), in_vmem(sums), b3m, w1m, w2m, b2m]
        + [in_hbm(x) for x in (third_m, w1, w2, b2, third, a0, a1, bu, b3, const)],
        [SMEM] + [VMEM] * 6 + [HBM] * 10,
        [jax.ShapeDtypeStruct((64, 48), F32), jax.ShapeDtypeStruct((1,), F32)],
        MID_SCRATCH
        + (
            pltpu.VMEM((224, 512), BF), pltpu.VMEM((432, 512), F32), pltpu.VMEM((216, 512), BF),
            pltpu.VMEM((2, 512, 224), BF), pltpu.VMEM((2, 512, 512), BF), pltpu.VMEM((2, 512, 128), F32), pltpu.VMEM((2, 432, 512), BF),
            pltpu.VMEM((48, 192), BF), pltpu.VMEM((48, 144), BF), pltpu.VMEM((2, 48, 128), F32), pltpu.VMEM((2, 48, 128), F32), pltpu.VMEM((8, 128), F32),
            pltpu.SemaphoreType.DMA((14,)),
        ),
        (VMEM, SMEM),
        limit=24 * 2**20,
    )


def body(images, *params):
    slots = lax.all_to_all(pack(images), ("rows", "chan"), 0, 0, tiled=True)
    third_mid = params[9].transpose(0, 1, 3, 2).reshape(3, 216, 512)
    third_top = params[20].transpose(0, 1, 3, 2).reshape(2, 432, 512)
    prepared = prep(params)
    where = lax.axis_index("rows").astype(jnp.int32).reshape(1)
    u, sums, latent = mid(where, slots, prepared, third_mid)
    latent_mid = lax.all_to_all(latent, "chan", 0, 0, tiled=True)
    latent_top, loglik = top(where, u, sums, prepared, third_mid, third_top)
    latent_top = latent_top.reshape(1, 4, 16, 48).transpose(0, 3, 1, 2)
    return latent_mid[:, :12, None, :32], latent_top, loglik


def solution(mesh):
    return jax.shard_map(
        body,
        mesh=mesh,
        in_specs=(P("batch", None, ("rows", "chan"), None),) + (P(),) * 22,
        out_specs=(
            P("batch", None, ("rows", "chan"), None),
            P(("batch", "chan"), None, "rows", None),
            P(("batch", "chan")),
        ),
        check_vma=False,
    )
```

```python
import functools
import math

import jax
import jax.numpy as jnp
from jax import lax
from jax.experimental import pallas as pl
from jax.experimental.pallas import tpu as pltpu
from jax.sharding import PartitionSpec as P

BF = jnp.bfloat16
F32 = jnp.float32
CHUNKS = 2
SIZE = 2048 // CHUNKS
log_two_pi = math.log(2.0 * math.pi)
VMEM = pl.BlockSpec(memory_space=pltpu.VMEM)
SMEM = pl.BlockSpec(memory_space=pltpu.SMEM)
HBM = pl.BlockSpec(memory_space=pltpu.HBM)


def iota(shape, dim):
    return lax.broadcasted_iota(jnp.int32, shape, dim)


def eye(n, dtype):
    return (iota((n, n), 0) == iota((n, n), 1)).astype(dtype)


def dot_t(a, b):
    return lax.dot_general(a, b, (((1,), (1,)), ((), ())), preferred_element_type=F32)


def dot(a, b):
    return jnp.dot(a, b, preferred_element_type=F32)


def halves(x):
    high = x.astype(BF)
    return high, (x - high.astype(F32)).astype(BF)


def to_column(row):
    n = row.shape[1]
    same = iota((n, n), 0) == iota((n, n), 1)
    return jnp.sum(jnp.where(same, row, 0.0), axis=1, keepdims=True)


def three_term_left(matrix):
    high, low = halves(matrix)
    return jnp.concatenate([high, high, low], axis=1)


def select_rows(n_out, n_in, source_of):
    return (iota((n_out, n_in), 1) == source_of(iota((n_out, n_in), 0))).astype(F32)


def spread_mid(o):
    return jnp.where(o < 12, o, jnp.where(o >= 20, o - 8, -1))


def flow_matrix(gain, lower, upper, diag, shift, n):
    i, j = iota((n, n), 0), iota((n, n), 1)
    low = jnp.where(i > j, lower, 0.0) + jnp.where(i == j, 1.0, 0.0)
    up = jnp.where(i < j, upper, 0.0) + jnp.where(i == j, jnp.exp(diag), 0.0)
    matrix = jnp.dot(low, up, precision=lax.Precision.HIGHEST, preferred_element_type=F32)
    matrix = matrix * jnp.exp(gain)
    return matrix, jnp.sum(matrix * shift, axis=1, keepdims=True)


def exact_dot(a, b):
    return jnp.dot(a, b, precision=lax.Precision.HIGHEST, preferred_element_type=F32)


def prep_kernel(
    shift_mid, gain_mid, lower_mid, upper_mid, diag_mid, first_mid, first_bias_mid, second_mid,
    second_bias_mid, third_bias_mid,
    shift_top, gain_top, lower_top, upper_top, diag_top, first_top, first_bias_top, second_top,
    second_bias_top, third_bias_top,
    a_mid, bu_mid, w1_mid, w2_mid, b2_mid, b3_mid,
    a_top0, a_top1, bu_top, w1_top, w2_top, b2_top, b3_top, const,
):
    hid = second_mid.shape[1]
    ident = eye(hid, BF)
    total = jnp.zeros((1, 1), F32)
    for s in range(3):
        row = slice(s, s + 1)
        matrix, offset = flow_matrix(gain_mid[row], lower_mid[s], upper_mid[s], diag_mid[row], shift_mid[row], 24)
        total = total + 2048.0 * jnp.sum(gain_mid[row] + diag_mid[row], axis=1, keepdims=True)
        rows = select_rows(32, 24, spread_mid)
        matrix = exact_dot(rows, matrix)
        offset = jnp.sum(rows * jnp.sum(jnp.where(eye(24, F32) > 0, offset, 0.0), axis=0, keepdims=True), axis=1, keepdims=True)
        offset = offset + (iota((32, 1), 0) == 12).astype(F32)
        if s == 0:
            held = iota((24, 32), 1)
            columns = (iota((24, 32), 0) == jnp.where(held % 8 < 6, held // 8 * 6 + held % 8, -1)).astype(F32)
        else:
            columns = (iota((24, 32), 0) == spread_mid(iota((24, 32), 1))).astype(F32)
        a_mid[s] = three_term_left(exact_dot(matrix, columns))
        bu_mid[s] = jnp.broadcast_to(offset, (32, 128))
        zeros = jnp.zeros((4, hid), F32)
        with_bias = jnp.concatenate([first_bias_mid[row].astype(F32), zeros[:3]], axis=0)
        blocks = []
        for tap in range(9):
            blocks += [first_mid[s, tap].astype(F32), with_bias if tap == 4 else zeros]
        w1_mid[s] = dot_t(ident, jnp.concatenate(blocks, axis=0).astype(BF)).astype(BF)
        w2_mid[s] = dot_t(ident, second_mid[s]).astype(BF)
        b2_mid[s] = jnp.broadcast_to(second_bias_mid[row], (8, hid))
        b3 = to_column(third_bias_mid[row]) + jnp.where(iota((24, 1), 0) < 12, 2.0, 0.0)
        b3_mid[s] = jnp.broadcast_to(b3, (24, 128))
    for s in range(2):
        row = slice(s, s + 1)
        matrix, offset = flow_matrix(gain_top[row], lower_top[s], upper_top[s], diag_top[row], shift_top[row], 48)
        total = total + 512.0 * jnp.sum(gain_top[row] + diag_top[row], axis=1, keepdims=True)
        if s == 0:
            k = iota((48, 64), 1)
            source = jnp.where(k % 16 >= 4, 4 * (k % 16 - 4) + k // 16, -1)
            a_top0[...] = three_term_left(exact_dot(matrix, (iota((48, 64), 0) == source).astype(F32)))
        else:
            a_top1[...] = three_term_left(matrix)
        bu_top[s] = jnp.broadcast_to(offset, (48, 128))
        blocks = [first_top[s, tap].astype(F32) for tap in range(9)]
        blocks += [first_bias_top[row].astype(F32), jnp.zeros((7, hid), F32)]
        w1_top[s] = dot_t(ident, jnp.concatenate(blocks, axis=0).astype(BF)).astype(BF)
        w2_top[s] = dot_t(ident, second_top[s]).astype(BF)
        b2_top[s] = jnp.broadcast_to(second_bias_top[row], (128, hid)).T
        b3 = to_column(third_bias_top[row]) + jnp.where(iota((48, 1), 0) < 24, 2.0, 0.0)
        b3_top[s] = jnp.broadcast_to(b3, (48, 128))
    const[...] = jnp.broadcast_to(total, (8, 128))


def tiled(column, lanes):
    return jnp.concatenate([column] * (lanes // 128), axis=1)


def moved(x, by):
    lanes = x.shape[1]
    return pltpu.roll(x, (-by) % lanes, 1)


def row_moved(x, dr, width):
    if dr == 0:
        return x
    lane = iota(x.shape, 1)
    inside = lane >= width if dr < 0 else lane < x.shape[1] - width
    return jnp.where(inside, moved(x, dr * width), 0.0)


def column_moved(x, dc, width):
    if dc == 0:
        return x
    column = iota(x.shape, 1) % width
    inside = column >= 1 if dc < 0 else column <= width - 2
    return jnp.where(inside, moved(x, dc), 0.0)


def conditioner(q, extra, refs, copies, width):
    cells = q.shape[1]
    sides = [column_moved(q, dc, width) for dc in (-1, 0, 1)]
    blocks = [row_moved(side, dr, width) for dr in (-1, 0, 1) for side in sides]
    x = jnp.concatenate(blocks + [extra], axis=0).astype(BF)
    awaited(copies)
    w1, w2, b2, w3, b3 = (ref[...] for ref in refs)
    inner = jnp.maximum(dot(w1, x), 0.0).astype(BF)
    middle = jnp.maximum(dot(w2, inner) + tiled(b2, cells), 0.0).astype(BF)
    p = dot(w3, middle)
    n_out = p.shape[0] // 9
    out = tiled(b3, cells)
    for dc in (-1, 0, 1):
        part = None
        for dr in (-1, 0, 1):
            tap = 3 * (dr + 1) + dc + 1
            term = row_moved(p[n_out * tap : n_out * (tap + 1), :], dr, width)
            part = term if part is None else part + term
        out = out + column_moved(part, dc, width)
    return out


def gate_of(g):
    e = jnp.exp(-jnp.abs(g))
    scale = 1.0 / (1.0 + e)
    return jnp.where(g >= 0.0, scale, e * scale), jnp.minimum(g, 0.0) - jnp.log(1.0 + e)


def mix(a, parts, bias):
    return dot(a, jnp.concatenate(parts, axis=0)) + bias


def widened(chunks, c):
    zeros = jnp.zeros((chunks[c].shape[0], 128), F32)
    low = chunks[c - 1][:, -128:] if c else zeros
    high = chunks[c + 1][:, :128] if c + 1 < CHUNKS else zeros
    return jnp.concatenate([low, chunks[c], high], axis=1)


def within(x):
    return x[:, 128 : 128 + SIZE]


def first_layer(u, c, w1):
    wide = widened([x[:16] for x in u] + [None] * (CHUNKS - len(u)), c)
    sides = [column_moved(wide, dc, 32) for dc in (-1, 0, 1)]
    blocks = [within(moved(side, 32 * dr) if dr else side) for dr in (-1, 0, 1) for side in sides]
    return jnp.maximum(dot(w1, jnp.concatenate(blocks, axis=0).astype(BF)), 0.0).astype(BF)


def last_layer(p, c, b3):
    wide = widened(p + [None] * (CHUNKS - len(p)), c)
    out = tiled(b3, SIZE)
    for dc in (-1, 0, 1):
        part = None
        for dr in (-1, 0, 1):
            tap = 3 * (dr + 1) + dc + 1
            term = wide[24 * tap : 24 * tap + 24]
            term = moved(term, 32 * dr) if dr else term
            part = term if part is None else part + term
        out = out + within(column_moved(part, dc, 32))
    return out


def mid_layers(u, inner, refs, copies, after):
    w2, bias, w3_ref, b3 = refs
    p, made, total = [], [], None

    def finish(c):
        out = last_layer(p, c, b3)
        scale, logs = gate_of(out[:16])
        updated = (u[c][16:] + out[8:]) * pltpu.roll(scale, 4, 0)
        made.append(after(jnp.concatenate([u[c][:16], updated], axis=0)))
        return logs

    middle = [jnp.maximum(dot(w2, x) + bias, 0.0).astype(BF) for x in inner]
    awaited(copies)
    for c in range(CHUNKS):
        p.append(dot(w3_ref[...], middle[c]))
        if c:
            logs = finish(c - 1)
            total = logs if total is None else total + logs
    return made, total, finish


def mid_steps(u, weights, copies, steps, mixes):
    w1, w2, b2, w3, b3 = weights
    inner = [first_layer(u, c, w1[steps[0]]) for c in range(CHUNKS)]
    total = None
    for n, s in enumerate(steps):
        bias = tiled(jnp.concatenate([b2[s]] * 16, axis=0).T, SIZE)
        made, logs, finish = mid_layers(u, inner, (w2[s], bias, w3.at[n], b3[s]), copies[n : n + 1], mixes[n])
        inner = []
        if n + 1 < len(steps):
            for c in range(CHUNKS - 2):
                inner.append(first_layer(made, c, w1[steps[n + 1]]))
        logs = logs + finish(CHUNKS - 1)
        total = logs if total is None else total + logs
        if n + 1 < len(steps):
            for c in range(CHUNKS - 2, CHUNKS):
                inner.append(first_layer(made, c, w1[steps[n + 1]]))
        u = made
    return u, jnp.sum(jnp.where(iota(total.shape, 0) < 12, total, 0.0), keepdims=True)


def next_mix(a, bu):
    def mixed(state):
        high, low = halves(state)
        return mix(a, [high, low, high], tiled(bu, state.shape[1]))

    return mixed


def started(pairs, sems):
    copies = [pltpu.make_async_copy(a, b, sems.at[k]) for k, (a, b) in enumerate(pairs)]
    for copy in copies:
        copy.start()
    return copies


def awaited(copies):
    for copy in copies:
        copy.wait()


def mid_kernel(where, slots, a_mid, bu_mid, b3, w1, w2, b2, w3h, u_out, sum_out, latent_out, w3, sems):
    copies = started([(w3h.at[s], w3.at[s]) for s in range(2)], sems)
    cells = 2048
    lane = iota((8, 128), 1) // 32
    groups = []
    for g in range(4):
        pieces = []
        for k in range(16):
            piece = None
            for j in range(4):
                source = jnp.concatenate([slots[8 * ((4 * k + j) % 8) + (4 * k + j) // 8, t] for t in range(3)] + [jnp.zeros((2, 128), F32)], axis=0)
                turn = (32 * (j - g)) % 128
                source = pltpu.roll(source, turn, 1) if turn else source
                piece = source if piece is None else jnp.where(lane == j, source, piece)
            pieces.append(piece)
        groups.append(jnp.concatenate(pieces, axis=1))
    state = jnp.concatenate(groups, axis=0)
    mixes = [next_mix(a_mid[s], bu_mid[s]) for s in range(3)]
    u = [mixes[0](state[:, SIZE * c : SIZE * (c + 1)]) for c in range(CHUNKS)]
    u, total = mid_steps(u, (w1, w2, b2, w3, b3), copies, (0, 1), mixes[1:])
    for c in range(CHUNKS):
        u_out[:, SIZE * c : SIZE * (c + 1)] = u[c]
    squares = sum(x[:16] * x[:16] for x in u)
    total = total - 0.5 * jnp.sum(jnp.where(iota(squares.shape, 0) < 12, squares, 0.0), keepdims=True)
    sum_out[...] = jnp.broadcast_to(total, (8, 128))
    own = u_out[0:16, pl.ds(pl.multiple_of(where[0] * 256, 256), 256)]
    for j in range(8):
        part = own[:, 128 * (j // 4) : 128 * (j // 4) + 128]
        latent_out[j] = pltpu.roll(part, 128 - 32 * (j % 4), 1) if j % 4 else part


def top_kernel(where, u_in, sum_in, b3m, w1m, w2m, b2m, w3mh, w1h, w2h, b2h, w3h, *rest):
    small_h, (latent_out, sum_out, w3m, w1, w2, b2, w3, *small, sems) = rest[:5], rest[5:]
    a_top0, a_top1, bu_top, b3, const = small
    pairs = [(w3mh.at[2], w3m.at[0])] + list(zip(small_h, small))
    for s in range(2):
        pairs += [(a.at[s], b.at[s]) for a, b in zip((w1h, w2h, b2h, w3h), (w1, w2, b2, w3))]
    copies = started(pairs, sems)
    u = [u_in[:, SIZE * c : SIZE * (c + 1)] for c in range(CHUNKS)]
    updated, logs = mid_steps(u, (w1m, w2m, b2m, w3m, b3m), copies[:1], (2,), [lambda state: state[16:]])
    updated = jnp.concatenate(updated, axis=1)
    awaited(copies[1:6])
    total = sum_in[0:1, 0:1] + const[0:1, 0:1] + logs
    high, low = halves(updated)
    cell = iota((128, 128), 0)
    target = 32 * (2 * (cell // 32 % 2) + cell % 2) + 16 * (cell // 64) + cell % 32 // 2
    order = (target == iota((128, 128), 1)).astype(BF)
    stacked = jnp.concatenate([part[:, 128 * k : 128 * k + 128] for part in (high, low) for k in range(16)], axis=0)
    stacked = dot(stacked, order)
    lane = iota((16, 128), 1) // 32
    parts = []
    for p in range(2):
        for ij in range(4):
            pieces = []
            for m in range(4):
                piece = None
                for j in range(4):
                    start = 256 * p + 16 * (4 * m + j)
                    source = stacked[start : start + 16]
                    turn = (32 * (j - ij)) % 128
                    source = pltpu.roll(source, turn, 1) if turn else source
                    piece = source if piece is None else jnp.where(lane == j, source, piece)
                pieces.append(piece)
            parts.append(jnp.concatenate(pieces, axis=1).astype(BF))
    u = mix(a_top0[...], parts + parts[:4], tiled(bu_top[0], 512))
    ones = (iota((8, 512), 0) == 0).astype(F32)
    for s in range(2):
        out = conditioner(u[:24], ones, (w1.at[s], w2.at[s], b2.at[s], w3.at[s], b3.at[s]), copies[6 + 4 * s : 10 + 4 * s], 16)
        scale, logs = gate_of(out[:24])
        total = total + jnp.sum(logs, keepdims=True)
        state = jnp.concatenate([u[:24], (u[24:] + out[24:]) * scale], axis=0)
        if s == 0:
            high, low = halves(state)
            u = mix(a_top1[...], [high, low, high], tiled(bu_top[1], 512))
    total = total - 0.5 * jnp.sum(state * state, keepdims=True)
    total = (total - 0.5 * log_two_pi * 49152.0) * (1.0 / 49152.0)
    sum_out[0] = total[0, 0]
    block = pltpu.roll(state, (512 - where[0] * 64) % 512, 1)
    block = jnp.concatenate([block[:, :128], jnp.zeros((80, 128), F32)], axis=0)
    latent_out[...] = block.T[:64, :48]


def pack_kernel(images, packed):
    for i in range(8):
        rows = images[i]
        wide = jnp.concatenate([rows[6 * j : 6 * j + 6] for j in range(4)], axis=1)
        for r in range(8):
            for t in range(3):
                packed[8 * i + r, t] = wide[2 * t : 2 * t + 2]


def shapes(*items):
    return tuple(jax.ShapeDtypeStruct(shape, dtype) for shape, dtype in items)


def in_vmem(x):
    return pltpu.with_memory_space_constraint(x, pltpu.VMEM)


def in_hbm(x):
    return pltpu.with_memory_space_constraint(x, pltpu.HBM)


def call(kernel, name, inputs, specs, outputs, scratch=(), out_specs=None, limit=None):
    return pl.pallas_call(
        kernel,
        in_specs=specs,
        out_specs=out_specs or (VMEM,) * len(outputs),
        out_shape=tuple(outputs),
        scratch_shapes=list(scratch),
        compiler_params=pltpu.CompilerParams(vmem_limit_bytes=limit),
        name=name,
    )(*inputs)


def pack(images):
    return pl.pallas_call(
        pack_kernel, in_specs=[VMEM], out_specs=VMEM, out_shape=jax.ShapeDtypeStruct((64, 3, 2, 128), F32), name="pack"
    )(images.reshape(8, 24, 32))


def prep(params):
    small = [p for i, p in enumerate(params) if i not in (9, 20)]
    return call(
        prep_kernel,
        "prep",
        small,
        [VMEM] * 20,
        (
            pltpu.VMEM((3, 32, 96), BF), pltpu.VMEM((3, 32, 128), F32), pltpu.VMEM((3, 512, 144), BF), pltpu.VMEM((3, 512, 512), BF),
            pltpu.VMEM((3, 8, 512), F32), pltpu.VMEM((3, 24, 128), F32),
        )
        + shapes(
            ((48, 192), BF), ((48, 144), BF), ((2, 48, 128), F32), ((2, 512, 224), BF), ((2, 512, 512), BF), ((2, 512, 128), F32),
            ((2, 48, 128), F32), ((8, 128), F32),
        ),
    )


def mid(where, slots, prepared, third):
    a, bu, w1, w2, b2, b3 = (in_vmem(x) for x in prepared[:6])
    return call(
        mid_kernel,
        "mid",
        [where, in_vmem(slots), a, bu, b3, w1, w2, b2, in_hbm(third)],
        [SMEM] + [VMEM] * 7 + [HBM],
        [pltpu.VMEM((32, 2048), F32), pltpu.VMEM((8, 128), F32), jax.ShapeDtypeStruct((8, 16, 128), F32)],
        (pltpu.VMEM((2, 216, 512), BF), pltpu.SemaphoreType.DMA((2,))),
        limit=24 * 2**20,
    )


def top(where, u, sums, prepared, third_m, third):
    w1m, w2m, b2m, b3m = (in_vmem(x) for x in prepared[2:6])
    a0, a1, bu, w1, w2, b2, b3, const = prepared[6:]
    return call(
        top_kernel,
        "top",
        [where, in_vmem(u), in_vmem(sums), b3m, w1m, w2m, b2m]
        + [in_hbm(x) for x in (third_m, w1, w2, b2, third, a0, a1, bu, b3, const)],
        [SMEM] + [VMEM] * 6 + [HBM] * 10,
        [jax.ShapeDtypeStruct((64, 48), F32), jax.ShapeDtypeStruct((1,), F32)],
        (
            pltpu.VMEM((1, 216, 512), BF),
            pltpu.VMEM((2, 512, 224), BF), pltpu.VMEM((2, 512, 512), BF), pltpu.VMEM((2, 512, 128), F32), pltpu.VMEM((2, 432, 512), BF),
            pltpu.VMEM((48, 192), BF), pltpu.VMEM((48, 144), BF), pltpu.VMEM((2, 48, 128), F32), pltpu.VMEM((2, 48, 128), F32), pltpu.VMEM((8, 128), F32),
            pltpu.SemaphoreType.DMA((14,)),
        ),
        (VMEM, SMEM),
        limit=24 * 2**20,
    )


def body(images, *params):
    slots = lax.all_to_all(pack(images), ("chan", "rows"), 0, 0, tiled=True)
    third_mid = params[9].transpose(0, 1, 3, 2).reshape(3, 216, 512)
    third_top = params[20].transpose(0, 1, 3, 2).reshape(2, 432, 512)
    prepared = prep(params)
    where = lax.axis_index("rows").astype(jnp.int32).reshape(1)
    u, sums, latent = mid(where, slots, prepared, third_mid)
    latent_mid = lax.all_to_all(latent, "chan", 0, 0, tiled=True)
    latent_top, loglik = top(where, u, sums, prepared, third_mid, third_top)
    latent_top = latent_top.reshape(1, 4, 16, 48).transpose(0, 3, 1, 2)
    return latent_mid[:, :12, None, :32], latent_top, loglik


def solution(mesh):
    return jax.shard_map(
        body,
        mesh=mesh,
        in_specs=(P("batch", None, ("rows", "chan"), None),) + (P(),) * 22,
        out_specs=(
            P("batch", None, ("rows", "chan"), None),
            P(("batch", "chan"), None, "rows", None),
            P(("batch", "chan")),
        ),
        check_vma=False,
    )
```

```python
import functools
import math

import jax
import jax.numpy as jnp
from jax import lax
from jax.experimental import pallas as pl
from jax.experimental.pallas import tpu as pltpu
from jax.sharding import PartitionSpec as P

BF = jnp.bfloat16
F32 = jnp.float32
CHUNKS = 2
MID_ROWS = 512
MID_OUT = 216
TOP_ROWS = 256
TOP_OUT = 216
SIZE = 2048 // CHUNKS
log_two_pi = math.log(2.0 * math.pi)
VMEM = pl.BlockSpec(memory_space=pltpu.VMEM)
SMEM = pl.BlockSpec(memory_space=pltpu.SMEM)
HBM = pl.BlockSpec(memory_space=pltpu.HBM)


def iota(shape, dim):
    return lax.broadcasted_iota(jnp.int32, shape, dim)


def eye(n, dtype):
    return (iota((n, n), 0) == iota((n, n), 1)).astype(dtype)


def dot_t(a, b):
    return lax.dot_general(a, b, (((1,), (1,)), ((), ())), preferred_element_type=F32)


def dot(a, b):
    return jnp.dot(a, b, preferred_element_type=F32)


def halves(x):
    high = x.astype(BF)
    return high, (x - high.astype(F32)).astype(BF)


def to_column(row):
    n = row.shape[1]
    same = iota((n, n), 0) == iota((n, n), 1)
    return jnp.sum(jnp.where(same, row, 0.0), axis=1, keepdims=True)


def three_term_left(matrix):
    high, low = halves(matrix)
    return jnp.concatenate([high, high, low], axis=1)


def select_rows(n_out, n_in, source_of):
    return (iota((n_out, n_in), 1) == source_of(iota((n_out, n_in), 0))).astype(F32)


def spread_mid(o):
    return jnp.where(o < 12, o, jnp.where(o >= 20, o - 8, -1))


def flow_matrix(gain, lower, upper, diag, shift, n):
    i, j = iota((n, n), 0), iota((n, n), 1)
    low = jnp.where(i > j, lower, 0.0) + jnp.where(i == j, 1.0, 0.0)
    up = jnp.where(i < j, upper, 0.0) + jnp.where(i == j, jnp.exp(diag), 0.0)
    matrix = jnp.dot(low, up, precision=lax.Precision.HIGHEST, preferred_element_type=F32)
    matrix = matrix * jnp.exp(gain)
    return matrix, jnp.sum(matrix * shift, axis=1, keepdims=True)


def exact_dot(a, b):
    return jnp.dot(a, b, precision=lax.Precision.HIGHEST, preferred_element_type=F32)


def prep_kernel(
    shift_mid, gain_mid, lower_mid, upper_mid, diag_mid, first_mid, first_bias_mid, second_mid,
    second_bias_mid, third_bias_mid,
    shift_top, gain_top, lower_top, upper_top, diag_top, first_top, first_bias_top, second_top,
    second_bias_top, third_bias_top,
    a_mid, bu_mid, w1_mid, w2_mid, b2_mid, b3_mid,
    a_top0, a_top1, bu_top, w1_top, w2_top, b2_top, b3_top, const,
):
    hid = second_mid.shape[1]
    ident = eye(hid, BF)
    total = jnp.zeros((1, 1), F32)
    for s in range(3):
        row = slice(s, s + 1)
        matrix, offset = flow_matrix(gain_mid[row], lower_mid[s], upper_mid[s], diag_mid[row], shift_mid[row], 24)
        total = total + 2048.0 * jnp.sum(gain_mid[row] + diag_mid[row], axis=1, keepdims=True)
        rows = select_rows(32, 24, spread_mid)
        matrix = exact_dot(rows, matrix)
        offset = jnp.sum(rows * jnp.sum(jnp.where(eye(24, F32) > 0, offset, 0.0), axis=0, keepdims=True), axis=1, keepdims=True)
        offset = offset + (iota((32, 1), 0) == 12).astype(F32)
        if s == 0:
            held = iota((24, 32), 1)
            columns = (iota((24, 32), 0) == jnp.where(held % 8 < 6, held // 8 * 6 + held % 8, -1)).astype(F32)
        else:
            columns = (iota((24, 32), 0) == spread_mid(iota((24, 32), 1))).astype(F32)
        a_mid[s] = three_term_left(exact_dot(matrix, columns))
        bu_mid[s] = jnp.broadcast_to(offset, (32, 128))
        zeros = jnp.zeros((4, hid), F32)
        with_bias = jnp.concatenate([first_bias_mid[row].astype(F32), zeros[:3]], axis=0)
        blocks = []
        for tap in range(9):
            blocks += [first_mid[s, tap].astype(F32), with_bias if tap == 4 else zeros]
        w1_mid[s] = dot_t(ident, jnp.concatenate(blocks, axis=0).astype(BF)).astype(BF)
        w2_mid[s] = dot_t(ident, second_mid[s]).astype(BF)
        b2_mid[s] = jnp.broadcast_to(second_bias_mid[row], (8, hid))
        b3 = to_column(third_bias_mid[row]) + jnp.where(iota((24, 1), 0) < 12, 2.0, 0.0)
        b3_mid[s] = jnp.broadcast_to(b3, (24, 128))
    for s in range(2):
        row = slice(s, s + 1)
        matrix, offset = flow_matrix(gain_top[row], lower_top[s], upper_top[s], diag_top[row], shift_top[row], 48)
        total = total + 512.0 * jnp.sum(gain_top[row] + diag_top[row], axis=1, keepdims=True)
        if s == 0:
            k = iota((48, 64), 1)
            source = jnp.where(k % 16 >= 4, 4 * (k % 16 - 4) + k // 16, -1)
            a_top0[...] = three_term_left(exact_dot(matrix, (iota((48, 64), 0) == source).astype(F32)))
        else:
            a_top1[...] = three_term_left(matrix)
        bu_top[s] = jnp.broadcast_to(offset, (48, 128))
        blocks = [first_top[s, tap].astype(F32) for tap in range(9)]
        blocks += [first_bias_top[row].astype(F32), jnp.zeros((7, hid), F32)]
        w1_top[s] = dot_t(ident, jnp.concatenate(blocks, axis=0).astype(BF)).astype(BF)
        w2_top[s] = dot_t(ident, second_top[s]).astype(BF)
        b2_top[s] = jnp.broadcast_to(second_bias_top[row], (128, hid)).T
        b3 = to_column(third_bias_top[row]) + jnp.where(iota((48, 1), 0) < 24, 2.0, 0.0)
        b3_top[s] = jnp.broadcast_to(b3, (48, 128))
    const[...] = jnp.broadcast_to(total, (8, 128))


def tiled(column, lanes):
    return jnp.concatenate([column] * (lanes // 128), axis=1)


def moved(x, by):
    lanes = x.shape[1]
    return pltpu.roll(x, (-by) % lanes, 1)


def row_moved(x, dr, width):
    if dr == 0:
        return x
    lane = iota(x.shape, 1)
    inside = lane >= width if dr < 0 else lane < x.shape[1] - width
    return jnp.where(inside, moved(x, dr * width), 0.0)


def column_moved(x, dc, width):
    if dc == 0:
        return x
    column = iota(x.shape, 1) % width
    inside = column >= 1 if dc < 0 else column <= width - 2
    return jnp.where(inside, moved(x, dc), 0.0)


def in_rows(a, b, rows, finish):
    return jnp.concatenate([finish(dot(a[k : k + rows], b), k) for k in range(0, a.shape[0], rows)], axis=0)


def conditioner(q, extra, refs, copies, width):
    cells = q.shape[1]
    sides = [column_moved(q, dc, width) for dc in (-1, 0, 1)]
    blocks = [row_moved(side, dr, width) for dr in (-1, 0, 1) for side in sides]
    x = jnp.concatenate(blocks + [extra], axis=0).astype(BF)
    awaited(copies)
    w1, w2, b2, w3, b3 = (ref[...] for ref in refs)
    inner = in_rows(w1, x, TOP_ROWS, lambda y, k: jnp.maximum(y, 0.0).astype(BF))
    middle = in_rows(w2, inner, TOP_ROWS, lambda y, k: jnp.maximum(y + tiled(b2[k : k + TOP_ROWS], cells), 0.0).astype(BF))
    p = in_rows(w3, middle, TOP_OUT, lambda y, k: y)
    n_out = p.shape[0] // 9
    out = tiled(b3, cells)
    for dc in (-1, 0, 1):
        part = None
        for dr in (-1, 0, 1):
            tap = 3 * (dr + 1) + dc + 1
            term = row_moved(p[n_out * tap : n_out * (tap + 1), :], dr, width)
            part = term if part is None else part + term
        out = out + column_moved(part, dc, width)
    return out


def gate_of(g):
    e = jnp.exp(-jnp.abs(g))
    scale = 1.0 / (1.0 + e)
    return jnp.where(g >= 0.0, scale, e * scale), jnp.minimum(g, 0.0) - jnp.log(1.0 + e)


def mix(a, parts, bias):
    return dot(a, jnp.concatenate(parts, axis=0)) + bias


def widened(chunks, c):
    zeros = jnp.zeros((chunks[c].shape[0], 128), F32)
    low = chunks[c - 1][:, -128:] if c else zeros
    high = chunks[c + 1][:, :128] if c + 1 < CHUNKS else zeros
    return jnp.concatenate([low, chunks[c], high], axis=1)


def within(x):
    return x[:, 128 : 128 + SIZE]


def first_layer(u, c, w1):
    wide = widened([x[:16] for x in u] + [None] * (CHUNKS - len(u)), c)
    sides = [column_moved(wide, dc, 32) for dc in (-1, 0, 1)]
    blocks = [within(moved(side, 32 * dr) if dr else side) for dr in (-1, 0, 1) for side in sides]
    return in_rows(w1, jnp.concatenate(blocks, axis=0).astype(BF), MID_ROWS, lambda y, k: jnp.maximum(y, 0.0).astype(BF))


def last_layer(p, c, b3):
    wide = widened(p + [None] * (CHUNKS - len(p)), c)
    out = tiled(b3, SIZE)
    for dc in (-1, 0, 1):
        part = None
        for dr in (-1, 0, 1):
            tap = 3 * (dr + 1) + dc + 1
            term = wide[24 * tap : 24 * tap + 24]
            term = moved(term, 32 * dr) if dr else term
            part = term if part is None else part + term
        out = out + within(column_moved(part, dc, 32))
    return out


def mid_layers(u, inner, refs, copies, after):
    w2, bias, w3_ref, b3 = refs
    p, made, total = [], [], None

    def finish(c):
        out = last_layer(p, c, b3)
        scale, logs = gate_of(out[:16])
        updated = (u[c][16:] + out[8:]) * pltpu.roll(scale, 4, 0)
        made.append(after(jnp.concatenate([u[c][:16], updated], axis=0)))
        return logs

    middle = [
        in_rows(w2, x, MID_ROWS, lambda y, k: jnp.maximum(y + bias[k : k + MID_ROWS], 0.0).astype(BF)) for x in inner
    ]
    awaited(copies)
    for c in range(CHUNKS):
        p.append(in_rows(w3_ref[...], middle[c], MID_OUT, lambda y, k: y))
        if c:
            logs = finish(c - 1)
            total = logs if total is None else total + logs
    return made, total, finish


def mid_steps(u, weights, copies, steps, mixes):
    w1, w2, b2, w3, b3 = weights
    inner = [first_layer(u, c, w1[steps[0]]) for c in range(CHUNKS)]
    total = None
    for n, s in enumerate(steps):
        bias = tiled(jnp.concatenate([b2[s]] * 16, axis=0).T, SIZE)
        made, logs, finish = mid_layers(u, inner, (w2[s], bias, w3.at[n], b3[s]), copies[n : n + 1], mixes[n])
        inner = []
        if n + 1 < len(steps):
            for c in range(CHUNKS - 2):
                inner.append(first_layer(made, c, w1[steps[n + 1]]))
        logs = logs + finish(CHUNKS - 1)
        total = logs if total is None else total + logs
        if n + 1 < len(steps):
            for c in range(CHUNKS - 2, CHUNKS):
                inner.append(first_layer(made, c, w1[steps[n + 1]]))
        u = made
    return u, jnp.sum(jnp.where(iota(total.shape, 0) < 12, total, 0.0), keepdims=True)


def next_mix(a, bu):
    def mixed(state):
        high, low = halves(state)
        return mix(a, [high, low, high], tiled(bu, state.shape[1]))

    return mixed


def started(pairs, sems):
    copies = [pltpu.make_async_copy(a, b, sems.at[k]) for k, (a, b) in enumerate(pairs)]
    for copy in copies:
        copy.start()
    return copies


def awaited(copies):
    for copy in copies:
        copy.wait()


def mid_kernel(where, slots, a_mid, bu_mid, b3, w1, w2, b2, w3h, u_out, sum_out, latent_out, w3, sems):
    copies = started([(w3h.at[s], w3.at[s]) for s in range(2)], sems)
    cells = 2048
    lane = iota((8, 128), 1) // 32
    groups = []
    for g in range(4):
        pieces = []
        for k in range(16):
            piece = None
            for j in range(4):
                source = jnp.concatenate([slots[8 * ((4 * k + j) % 8) + (4 * k + j) // 8, t] for t in range(3)] + [jnp.zeros((2, 128), F32)], axis=0)
                turn = (32 * (j - g)) % 128
                source = pltpu.roll(source, turn, 1) if turn else source
                piece = source if piece is None else jnp.where(lane == j, source, piece)
            pieces.append(piece)
        groups.append(jnp.concatenate(pieces, axis=1))
    state = jnp.concatenate(groups, axis=0)
    mixes = [next_mix(a_mid[s], bu_mid[s]) for s in range(3)]
    u = [mixes[0](state[:, SIZE * c : SIZE * (c + 1)]) for c in range(CHUNKS)]
    u, total = mid_steps(u, (w1, w2, b2, w3, b3), copies, (0, 1), mixes[1:])
    for c in range(CHUNKS):
        u_out[:, SIZE * c : SIZE * (c + 1)] = u[c]
    squares = sum(x[:16] * x[:16] for x in u)
    total = total - 0.5 * jnp.sum(jnp.where(iota(squares.shape, 0) < 12, squares, 0.0), keepdims=True)
    sum_out[...] = jnp.broadcast_to(total, (8, 128))
    own = u_out[0:16, pl.ds(pl.multiple_of(where[0] * 256, 256), 256)]
    for j in range(8):
        part = own[:, 128 * (j // 4) : 128 * (j // 4) + 128]
        latent_out[j] = pltpu.roll(part, 128 - 32 * (j % 4), 1) if j % 4 else part


def top_kernel(where, u_in, sum_in, b3m, w1m, w2m, b2m, w3mh, w1h, w2h, b2h, w3h, *rest):
    small_h, (latent_out, sum_out, w3m, w1, w2, b2, w3, *small, sems) = rest[:5], rest[5:]
    a_top0, a_top1, bu_top, b3, const = small
    pairs = [(w3mh.at[2], w3m.at[0])] + list(zip(small_h, small))
    for s in range(2):
        pairs += [(a.at[s], b.at[s]) for a, b in zip((w1h, w2h, b2h, w3h), (w1, w2, b2, w3))]
    copies = started(pairs, sems)
    u = [u_in[:, SIZE * c : SIZE * (c + 1)] for c in range(CHUNKS)]
    updated, logs = mid_steps(u, (w1m, w2m, b2m, w3m, b3m), copies[:1], (2,), [lambda state: state[16:]])
    updated = jnp.concatenate(updated, axis=1)
    awaited(copies[1:6])
    total = sum_in[0:1, 0:1] + const[0:1, 0:1] + logs
    high, low = halves(updated)
    cell = iota((128, 128), 0)
    target = 32 * (2 * (cell // 32 % 2) + cell % 2) + 16 * (cell // 64) + cell % 32 // 2
    order = (target == iota((128, 128), 1)).astype(BF)
    stacked = jnp.concatenate([part[:, 128 * k : 128 * k + 128] for part in (high, low) for k in range(16)], axis=0)
    stacked = dot(stacked, order)
    lane = iota((16, 128), 1) // 32
    parts = []
    for p in range(2):
        for ij in range(4):
            pieces = []
            for m in range(4):
                piece = None
                for j in range(4):
                    start = 256 * p + 16 * (4 * m + j)
                    source = stacked[start : start + 16]
                    turn = (32 * (j - ij)) % 128
                    source = pltpu.roll(source, turn, 1) if turn else source
                    piece = source if piece is None else jnp.where(lane == j, source, piece)
                pieces.append(piece)
            parts.append(jnp.concatenate(pieces, axis=1).astype(BF))
    u = mix(a_top0[...], parts + parts[:4], tiled(bu_top[0], 512))
    ones = (iota((8, 512), 0) == 0).astype(F32)
    for s in range(2):
        out = conditioner(u[:24], ones, (w1.at[s], w2.at[s], b2.at[s], w3.at[s], b3.at[s]), copies[6 + 4 * s : 10 + 4 * s], 16)
        scale, logs = gate_of(out[:24])
        total = total + jnp.sum(logs, keepdims=True)
        state = jnp.concatenate([u[:24], (u[24:] + out[24:]) * scale], axis=0)
        if s == 0:
            high, low = halves(state)
            u = mix(a_top1[...], [high, low, high], tiled(bu_top[1], 512))
    total = total - 0.5 * jnp.sum(state * state, keepdims=True)
    total = (total - 0.5 * log_two_pi * 49152.0) * (1.0 / 49152.0)
    sum_out[0] = total[0, 0]
    block = pltpu.roll(state, (512 - where[0] * 64) % 512, 1)
    block = jnp.concatenate([block[:, :128], jnp.zeros((80, 128), F32)], axis=0)
    latent_out[...] = block.T[:64, :48]


def pack_kernel(images, packed):
    for i in range(8):
        rows = images[i]
        wide = jnp.concatenate([rows[6 * j : 6 * j + 6] for j in range(4)], axis=1)
        for r in range(8):
            for t in range(3):
                packed[8 * i + r, t] = wide[2 * t : 2 * t + 2]


def shapes(*items):
    return tuple(jax.ShapeDtypeStruct(shape, dtype) for shape, dtype in items)


def in_vmem(x):
    return pltpu.with_memory_space_constraint(x, pltpu.VMEM)


def in_hbm(x):
    return pltpu.with_memory_space_constraint(x, pltpu.HBM)


def call(kernel, name, inputs, specs, outputs, scratch=(), out_specs=None, limit=None):
    return pl.pallas_call(
        kernel,
        in_specs=specs,
        out_specs=out_specs or (VMEM,) * len(outputs),
        out_shape=tuple(outputs),
        scratch_shapes=list(scratch),
        compiler_params=pltpu.CompilerParams(vmem_limit_bytes=limit),
        name=name,
    )(*inputs)


def pack(images):
    return pl.pallas_call(
        pack_kernel, in_specs=[VMEM], out_specs=VMEM, out_shape=jax.ShapeDtypeStruct((64, 3, 2, 128), F32), name="pack"
    )(images.reshape(8, 24, 32))


def prep(params):
    small = [p for i, p in enumerate(params) if i not in (9, 20)]
    return call(
        prep_kernel,
        "prep",
        small,
        [VMEM] * 20,
        (
            pltpu.VMEM((3, 32, 96), BF), pltpu.VMEM((3, 32, 128), F32), pltpu.VMEM((3, 512, 144), BF), pltpu.VMEM((3, 512, 512), BF),
            pltpu.VMEM((3, 8, 512), F32), pltpu.VMEM((3, 24, 128), F32),
        )
        + shapes(
            ((48, 192), BF), ((48, 144), BF), ((2, 48, 128), F32), ((2, 512, 224), BF), ((2, 512, 512), BF), ((2, 512, 128), F32),
            ((2, 48, 128), F32), ((8, 128), F32),
        ),
    )


def mid(where, slots, prepared, third):
    a, bu, w1, w2, b2, b3 = (in_vmem(x) for x in prepared[:6])
    return call(
        mid_kernel,
        "mid",
        [where, in_vmem(slots), a, bu, b3, w1, w2, b2, in_hbm(third)],
        [SMEM] + [VMEM] * 7 + [HBM],
        [pltpu.VMEM((32, 2048), F32), pltpu.VMEM((8, 128), F32), jax.ShapeDtypeStruct((8, 16, 128), F32)],
        (pltpu.VMEM((2, 216, 512), BF), pltpu.SemaphoreType.DMA((2,))),
        limit=24 * 2**20,
    )


def top(where, u, sums, prepared, third_m, third):
    w1m, w2m, b2m, b3m = (in_vmem(x) for x in prepared[2:6])
    a0, a1, bu, w1, w2, b2, b3, const = prepared[6:]
    return call(
        top_kernel,
        "top",
        [where, in_vmem(u), in_vmem(sums), b3m, w1m, w2m, b2m]
        + [in_hbm(x) for x in (third_m, w1, w2, b2, third, a0, a1, bu, b3, const)],
        [SMEM] + [VMEM] * 6 + [HBM] * 10,
        [jax.ShapeDtypeStruct((64, 48), F32), jax.ShapeDtypeStruct((1,), F32)],
        (
            pltpu.VMEM((1, 216, 512), BF),
            pltpu.VMEM((2, 512, 224), BF), pltpu.VMEM((2, 512, 512), BF), pltpu.VMEM((2, 512, 128), F32), pltpu.VMEM((2, 432, 512), BF),
            pltpu.VMEM((48, 192), BF), pltpu.VMEM((48, 144), BF), pltpu.VMEM((2, 48, 128), F32), pltpu.VMEM((2, 48, 128), F32), pltpu.VMEM((8, 128), F32),
            pltpu.SemaphoreType.DMA((14,)),
        ),
        (VMEM, SMEM),
        limit=24 * 2**20,
    )


def body(images, *params):
    slots = lax.all_to_all(pack(images), ("chan", "rows"), 0, 0, tiled=True)
    third_mid = params[9].transpose(0, 1, 3, 2).reshape(3, 216, 512)
    third_top = params[20].transpose(0, 1, 3, 2).reshape(2, 432, 512)
    prepared = prep(params)
    where = lax.axis_index("rows").astype(jnp.int32).reshape(1)
    u, sums, latent = mid(where, slots, prepared, third_mid)
    latent_mid = lax.all_to_all(latent, "chan", 0, 0, tiled=True)
    latent_top, loglik = top(where, u, sums, prepared, third_mid, third_top)
    latent_top = latent_top.reshape(1, 4, 16, 48).transpose(0, 3, 1, 2)
    return latent_mid[:, :12, None, :32], latent_top, loglik


def solution(mesh):
    return jax.shard_map(
        body,
        mesh=mesh,
        in_specs=(P("batch", None, ("rows", "chan"), None),) + (P(),) * 22,
        out_specs=(
            P("batch", None, ("rows", "chan"), None),
            P(("batch", "chan"), None, "rows", None),
            P(("batch", "chan")),
        ),
        check_vma=False,
    )
```
